32 devices in a mesh: gx: 8 (over y, x, core), gy: 4 (over z).
Axes of the slice: x: 2, y: 2, z: 4, core: 2. Of those that a mesh axis runs over, the one named last changes fastest.
Arguments:
- basis: float32 [32, 128, 64, 256], P(None, 'gx', 'gy'), may hold values from -0.09375 to 0.09375
- reaction: float32 [128, 64, 256], P('gx', 'gy'), may hold values from 0.5 to 4
Outputs:
- extended: float32 [32, 128, 64, 256], P(None, 'gx', 'gy')
- coarse: float32 [32, 5, 32, 32], replicated
The draws below stay inside these ranges and needn't reach their ends.
All inputs are finite; a program needn't handle non-finite values.
Results may differ from the reference program's by a relative error of at most 0.000071.
Values sent between devices are 32-bit elements; how exact they have to be, the bound alone decides.
A program may use at most 128 MiB of HBM per device.

```python
import math
import jax
import jax.numpy as jnp
from jax import lax

K = 32
SWEEPS = 4
CX = 16
CY = 16
CZ = 256
NX = 128
NY = 64
N_GX = 8
N_GY = 4


def level_of(rng, extent, shards, smallest, high):
    factor_of, own = 1.0, jax.random.fold_in(rng, 6)
    for axis_at, blocks in shards:
        draws = jnp.exp(jax.random.uniform(jax.random.fold_in(own, axis_at), (blocks,), jnp.float32, smallest / len(shards), high / len(shards)))
        factor_of = factor_of * jnp.repeat(draws, extent[axis_at] // blocks).reshape([-1 if axis == axis_at else 1 for axis in range(len(extent))])
    return factor_of


def centred(rng, extent, width, limit, shards=(), dtype=jnp.bfloat16):
    loudness = level_of(rng, extent, shards, -0.22, 0.18) if shards else 1.0
    result = jax.random.normal(rng, extent, jnp.float32) * width * loudness
    return jnp.minimum(jnp.maximum(result, -limit), limit).astype(dtype)


def setup_inputs(seed: int = 0) -> dict:
    keys = jax.random.split(jax.random.key(seed), 3)
    basis = centred(keys[0], (K, NX, NY, CZ), (CY * CZ) ** -0.5, 0.09375, ((1, 8), (2, 4)), jnp.float32)
    reaction = jnp.clip(jnp.exp(math.log(4.0) - 2.0794415 * jax.random.uniform(keys[1], (NX, NY, CZ), jnp.float32) ** level_of(keys[1], (NX, NY, CZ), ((0, 8), (1, 4)), -0.2, 0.2)), 0.5, 4.0)
    return dict(basis=basis, reaction=reaction)


OMEGA = 0.8


def stencil(field, coef):
    padded = jnp.pad(field, ((0, 0), (1, 1), (1, 1), (1, 1)))
    beside = padded[:, 2:, 1:-1, 1:-1] + padded[:, :-2, 1:-1, 1:-1]
    beside = beside + padded[:, 1:-1, 2:, 1:-1] + padded[:, 1:-1, :-2, 1:-1]
    beside = beside + padded[:, 1:-1, 1:-1, 2:] + padded[:, 1:-1, 1:-1, :-2]
    return (6.0 + coef) * field - beside


def extend_one(pair):
    phi, coef = pair
    kk, cx, cy, cz = phi.shape
    xpos = lax.broadcasted_iota(jnp.int32, (cx, cy, cz), 0)
    ypos = lax.broadcasted_iota(jnp.int32, (cx, cy, cz), 1)
    inner = (xpos >= 1) & (xpos <= cx - 2) & (ypos >= 1) & (ypos <= cy - 2)
    for sweep in range(SWEEPS):
        update = OMEGA * stencil(phi, coef) / (6.0 + coef)
        phi = phi - jnp.where(inner[None], update, jnp.float32(0.0))
    applied = stencil(phi, coef)
    diag = jnp.dot(phi.reshape(kk, -1), applied.reshape(kk, -1).T,
                   precision=lax.Precision.HIGHEST, preferred_element_type=jnp.float32)
    return phi, diag


def couple(own, other):
    return -jnp.einsum("iabyz,jabyz->abij", own, other, precision=lax.Precision.HIGHEST)


def reference(basis, reaction):
    gxn, gyn = N_GX, N_GY
    blocked = basis.reshape(K, gxn, CX, gyn, CY, CZ)
    subs = blocked.transpose(1, 3, 0, 2, 4, 5).reshape(gxn * gyn, K, CX, CY, CZ)
    coefs = reaction.reshape(gxn, CX, gyn, CY, CZ).transpose(0, 2, 1, 3, 4).reshape(gxn * gyn, CX, CY, CZ)
    phis, diags = lax.map(extend_one, (subs, coefs))
    extended = phis.reshape(gxn, gyn, K, CX, CY, CZ).transpose(2, 0, 3, 1, 4, 5).reshape(K, gxn * CX, gyn * CY, CZ)
    low_x = blocked[:, :, 0]
    high_x = blocked[:, :, CX - 1]
    zero_x = jnp.zeros_like(low_x[:, :1])
    minus_x = couple(low_x, jnp.concatenate([zero_x, high_x[:, :-1]], axis=1))
    plus_x = couple(high_x, jnp.concatenate([low_x[:, 1:], zero_x], axis=1))
    low_y = blocked[:, :, :, :, 0].transpose(0, 1, 3, 2, 4)
    high_y = blocked[:, :, :, :, CY - 1].transpose(0, 1, 3, 2, 4)
    zero_y = jnp.zeros_like(low_y[:, :, :1])
    minus_y = couple(low_y, jnp.concatenate([zero_y, high_y[:, :, :-1]], axis=2))
    plus_y = couple(high_y, jnp.concatenate([low_y[:, :, 1:], zero_y], axis=2))
    count = gxn * gyn
    coarse = jnp.stack([diags, minus_x.reshape(count, K, K), plus_x.reshape(count, K, K),
                        minus_y.reshape(count, K, K), plus_y.reshape(count, K, K)], axis=1)
    return extended, coarse
```

```python
import functools

import jax
import jax.numpy as jnp
from jax import lax
from jax.experimental import pallas as pl
from jax.experimental.pallas import tpu as pltpu
from jax.sharding import PartitionSpec as P

SWEEPS = 4
OMEGA = 0.8
ROWS = 8
LANES = 128
MESH = pl.DeviceIdType.MESH
F32 = jnp.float32
BF16 = jnp.bfloat16


def split(value):
    high = value.astype(BF16)
    low = (value - high.astype(F32)).astype(BF16)
    return high, low


def thirds(value):
    first = value.astype(BF16)
    rest = value - first.astype(F32)
    second = rest.astype(BF16)
    third = (rest - second.astype(F32)).astype(BF16)
    return jnp.concatenate([first, second, third], axis=0)


def block_sum(square, width):
    half = square.shape[0] // 2
    full = square[:half, :half] + square[:half, half:] + square[half:, :half]
    total = full[:width, :width]
    for i in range(width, half, width):
        total = total + full[i:i + width, i:i + width]
    return total


def packed(block):
    rows = block.shape[0] * block.shape[1] // LANES
    return jnp.concatenate(
        [block[i:i + rows] for i in range(0, block.shape[0], rows)], axis=1
    )


def unpacked(tile, width):
    return jnp.concatenate(
        [tile[:, i:i + width] for i in range(0, LANES, width)], axis=0
    )


def main_kernel(
    ngx, ngy, basis, reaction, nat, tiles,
    react, spread, weight, centre, first, second, left0, left1, right0, right1,
    gram, face_x, face_y, held,
    in_sem, react_sem, face_send, face_recv, send_y, recv_y, send_x, recv_x,
):
    width, cx, cy, cz = basis.shape
    yo = LANES // width
    yi = cy // yo
    group = cx // yo
    halves = cz // LANES
    ztiles = cz // ROWS
    gx, gy = lax.axis_index("gx"), lax.axis_index("gy")

    barrier = pltpu.get_barrier_semaphore()
    for d in range(1, ngy):
        pl.semaphore_signal(barrier, inc=1, device_id=(gx, lax.rem(gy + d, ngy)), device_id_type=MESH)
    for d in range(1, ngx):
        pl.semaphore_signal(barrier, inc=1, device_id=(lax.rem(gx + d, ngx), gy), device_id_type=MESH)

    load = pltpu.make_async_copy(reaction, react, react_sem)
    load.start()

    @pl.loop(0, cx)
    def _(x):
        for y in range(cy):
            pltpu.make_async_copy(
                basis.at[:, x, y, :],
                nat.at[x, y % yi, pl.ds((y // yi) * width, width), :],
                in_sem.at[x],
            ).start()

    def arrived(x):
        pltpu.make_async_copy(nat.at[x], nat.at[x], in_sem.at[x]).wait()

    def over_x(peer):
        return pltpu.make_async_remote_copy(
            src_ref=nat.at[0], dst_ref=face_x, send_sem=face_send.at[0], recv_sem=face_recv.at[0],
            device_id=(peer, gy), device_id_type=MESH,
        )

    def over_y(x, peer):
        return pltpu.make_async_remote_copy(
            src_ref=nat.at[x, 0, pl.ds(0, width), :],
            dst_ref=face_y.at[x // yo, pl.ds(lax.rem(x, yo) * width, width), :],
            send_sem=face_send.at[1], recv_sem=face_recv.at[1],
            device_id=(gx, peer), device_id_type=MESH,
        )

    rows = lax.broadcasted_iota(jnp.int32, (cy, yi * LANES), 0)
    cols = lax.broadcasted_iota(jnp.int32, (cy, yi * LANES), 1)
    chosen = rows == (lax.rem(cols, LANES) // width) * yi + cols // LANES
    pick = jnp.where(chosen, 1.0, 0.0).astype(BF16)
    spread[...] = jnp.concatenate([pick, pick, pick], axis=0)

    blank = jnp.zeros((ROWS, LANES), F32)
    for buffer in (first, second):
        @pl.loop(0, cx)
        def _(x):
            for j in range(yi):
                buffer[x, j, 0:ROWS, :] = blank
                buffer[x, j, cz + ROWS:cz + 2 * ROWS, :] = blank

    left1[...] = jnp.zeros_like(left1)
    right1[...] = jnp.zeros_like(right1)
    gram[...] = jnp.zeros_like(gram)

    def expanded(values):
        return lax.dot_general(
            thirds(values), spread[...], (((0,), (0,)), ((), ())), preferred_element_type=F32
        )

    load.wait()
    line = lax.broadcasted_iota(jnp.int32, (cy, cz), 0)
    face_row = (line == 0) | (line == cy - 1)

    @pl.loop(1, cx - 1)
    def _(x):
        scaled = jnp.where(face_row, 0.0, OMEGA / (6.0 + react[x]))
        wide = expanded(scaled)
        for j in range(yi):
            weight[x, j] = wide[:, j * LANES:(j + 1) * LANES]

    pl.semaphore_wait(barrier, ngx + ngy - 2)

    lane = lax.broadcasted_iota(jnp.int32, (ROWS, LANES), 1)
    keep = [jnp.full((ROWS, LANES), 1.0 - OMEGA, F32) for _ in range(yi)]
    keep[0] = jnp.where(lane < width, 1.0, keep[0])
    keep[yi - 1] = jnp.where(lane >= LANES - width, 1.0, keep[yi - 1])

    def take_in(x):
        arrived(x)

        @pl.when(gy > 0)
        def _():
            over_y(x, gy - 1).start()

        for j in range(yi):
            for h in range(halves):
                part = nat[x, j, :, h * LANES:(h + 1) * LANES]
                first[x, j, ROWS + h * LANES:ROWS + (h + 1) * LANES, :] = part.T

    def line_of(ref, x, t, shift=0):
        return [ref[x, j, pl.ds(ROWS + t * ROWS + shift, ROWS), :] for j in range(yi)]

    def ring(values):
        before = pltpu.roll(values[yi - 1], width, 1)
        after = pltpu.roll(values[0], LANES - width, 1)
        return [before] + values + [after]

    def update(source, target, x, t, down, here, up):
        near = ring(here)
        below, above = line_of(source, x, t, -1), line_of(source, x, t, 1)
        out = []
        for j in range(yi):
            total = (down[j] + up[j]) + (near[j] + near[j + 2]) + (below[j] + above[j])
            value = keep[j] * here[j] + weight[x, j, pl.ds(t * ROWS, ROWS), :] * total
            target[x, j, pl.ds(ROWS + t * ROWS, ROWS), :] = value
            out.append(value)
        return out

    def sweep_row(source, target, x):
        for t in range(ztiles):
            update(
                source, target, x, t,
                line_of(source, x - 1, t), line_of(source, x, t), line_of(source, x + 1, t),
            )

    def sweep(source, target):
        @pl.loop(0, ztiles, unroll=2)
        def _(t):
            down, here = line_of(source, 0, t), line_of(source, 1, t)
            for x in range(1, cx - 1):
                up = line_of(source, x + 1, t)
                update(source, target, x, t, down, here, up)
                down, here = here, up

    take_in(0)

    @pl.when(gx > 0)
    def _():
        over_x(gx - 1).start()

    take_in(1)
    take_in(2)

    @pl.loop(3, cx)
    def _(x):
        take_in(x)
        sweep_row(first, second, x - 2)

    sweep_row(first, second, cx - 2)

    @pl.loop(0, ztiles)
    def _(t):
        for x in (0, cx - 1):
            for j, value in enumerate(line_of(first, x, t)):
                second[x, j, pl.ds(ROWS + t * ROWS, ROWS), :] = value

    sweep(second, first)
    sweep(first, second)

    def couple():
        return -block_sum(
            lax.dot_general(
                left0[...], left1[...], (((1,), (1,)), ((), ())), preferred_element_type=F32
            ),
            width,
        )

    def fill(ref, row, column, value):
        high, low = split(value)
        size = value.shape[0]
        ref[row:row + size, column * cz:(column + 1) * cz] = high
        ref[LANES + row:LANES + row + size, column * cz:(column + 1) * cz] = low

    @pl.when(gx < ngx - 1)
    def _():
        over_x(gx).wait_recv()

    for j in range(yi):
        fill(left0, 0, j, nat[cx - 1, j])
        fill(left1, 0, j, face_x[j])
    plus_x = couple()
    held[gx, gy, 1] = packed(plus_x)
    held[gx, gy, 2] = packed(plus_x.T)

    @pl.when(gy < ngy - 1)
    def _():
        pltpu.make_async_copy(face_y, face_y, face_recv.at[1]).wait()

    for x in range(cx):
        fill(left0, (x % yo) * width, x // yo, nat[x, yi - 1, LANES - width:, :])
    for j in range(group):
        fill(left1, 0, j, face_y[j])
    plus_y = couple()
    held[gx, gy, 3] = packed(plus_y)
    held[gx, gy, 4] = packed(plus_y.T)

    @pl.when(gx > 0)
    def _():
        over_x(gx).wait_send()

    @pl.when(gy > 0)
    def _():
        pltpu.make_async_copy(face_y, face_y, face_send.at[1]).wait()

    left1[...] = jnp.zeros_like(left1)

    def product(x, left, right, last=False):
        wide = expanded(3.0 + 0.5 * react[x])
        for j in range(yi):
            centre[j] = wide[:, j * LANES:(j + 1) * LANES]
        for t in range(ztiles):
            here = line_of(second_out, x, t)
            above = line_of(second_out, x, t, 1)
            up = None if last else line_of(second_out, x + 1, t)
            edge = jnp.where(
                lane >= LANES - width, 0.0, pltpu.roll(here[0], LANES - width, 1)
            )
            beside = here[1:] + [edge]
            for j in range(yi):
                total = beside[j] + above[j]
                if up is not None:
                    total = total + up[j]
                applied = centre[j, t * ROWS:(t + 1) * ROWS, :] * here[j] - total
                work[j, t * ROWS:(t + 1) * ROWS, :] = applied
        for j in range(yi):
            high, low = split(work[j])
            right[j * cz:(j + 1) * cz, :LANES] = high
            right[j * cz:(j + 1) * cz, LANES:] = low
            for h in range(halves):
                part = second_out[x, j, ROWS + h * LANES:ROWS + (h + 1) * LANES, :].T
                nat[x, j, :, h * LANES:(h + 1) * LANES] = part
                high, low = split(part)
                left[:LANES, j * cz + h * LANES:j * cz + (h + 1) * LANES] = high
                left[LANES:, j * cz + h * LANES:j * cz + (h + 1) * LANES] = low

    def gather_product(left, right):
        gram[...] += jnp.dot(left[...], right[...], preferred_element_type=F32)

    source, second_out = second, first
    work = centre

    @pl.loop(0, cx - 2, step=2)
    def _(x):
        gather_product(left1, right1)
        sweep_row(source, second_out, x + 1)
        product(x, left0, right0)
        gather_product(left0, right0)
        sweep_row(source, second_out, x + 2)
        product(x + 1, left1, right1)

    gather_product(left1, right1)
    product(cx - 2, left0, right0)
    gather_product(left0, right0)
    product(cx - 1, left1, right1, last=True)
    gather_product(left1, right1)

    half = block_sum(gram[...], width)
    held[gx, gy, 0] = packed(half + half.T)

    def to_y(owner, peer):
        piece = held.at[gx, owner]
        return pltpu.make_async_remote_copy(
            src_ref=piece, dst_ref=piece, send_sem=send_y.at[peer], recv_sem=recv_y.at[owner],
            device_id=(gx, peer), device_id_type=MESH,
        )

    def to_x(row, owner, peer):
        piece = held.at[row, owner]
        return pltpu.make_async_remote_copy(
            src_ref=piece, dst_ref=piece, send_sem=send_x.at[peer, owner], recv_sem=recv_x.at[row, owner],
            device_id=(peer, gy), device_id_type=MESH,
        )

    for d in range(1, ngy):
        to_y(gy, lax.rem(gy + d, ngy)).start()
    for d in range(1, ngx):
        to_x(gx, gy, lax.rem(gx + d, ngx)).start()
    for d in range(1, ngy):
        owner = lax.rem(gy + d, ngy)
        to_y(owner, owner).wait_recv()
        for e in range(1, ngx):
            to_x(gx, owner, lax.rem(gx + e, ngx)).start()
    for d in range(ngy):
        owner = lax.rem(gy + d, ngy)
        for e in range(1, ngx):
            row = lax.rem(gx + e, ngx)
            to_x(row, owner, row).wait_recv()
    for d in range(1, ngy):
        to_y(gy, lax.rem(gy + d, ngy)).wait_send()
    for d in range(ngy):
        owner = lax.rem(gy + d, ngy)
        for e in range(1, ngx):
            to_x(gx, owner, lax.rem(gx + e, ngx)).wait_send()
    tiles[...] = held[...]


def main(basis, reaction):
    ngx, ngy = lax.axis_size("gx"), lax.axis_size("gy")
    width, cx, cy, cz = basis.shape
    yo = LANES // width
    yi = cy // yo
    hbm = pl.BlockSpec(memory_space=pltpu.HBM)
    vmem = pl.BlockSpec(memory_space=pltpu.VMEM)
    field = pltpu.VMEM((cx, yi, cz + 2 * ROWS, LANES), F32)
    left = pltpu.VMEM((2 * LANES, yi * cz), BF16)
    right = pltpu.VMEM((yi * cz, 2 * LANES), BF16)
    held = (ngx, ngy, 5, width * width // LANES, LANES)
    return pl.pallas_call(
        functools.partial(main_kernel, ngx, ngy),
        in_specs=[hbm, hbm],
        out_specs=[vmem, vmem],
        out_shape=[
            jax.ShapeDtypeStruct((cx, yi, LANES, cz), F32),
            jax.ShapeDtypeStruct(held, F32),
        ],
        scratch_shapes=[
            pltpu.VMEM((cx, cy, cz), F32),
            pltpu.VMEM((3 * cy, yi * LANES), BF16),
            pltpu.VMEM((cx, yi, cz, LANES), F32),
            pltpu.VMEM((yi, cz, LANES), F32),
            field, field, left, left, right, right,
            pltpu.VMEM((2 * LANES, 2 * LANES), F32),
            pltpu.VMEM((yi, LANES, cz), F32),
            pltpu.VMEM((cx // yo, LANES, cz), F32),
            pltpu.VMEM(held, F32),
            pltpu.SemaphoreType.DMA((cx,)),
            pltpu.SemaphoreType.DMA,
            pltpu.SemaphoreType.DMA((2,)),
            pltpu.SemaphoreType.DMA((2,)),
            pltpu.SemaphoreType.DMA((ngy,)),
            pltpu.SemaphoreType.DMA((ngy,)),
            pltpu.SemaphoreType.DMA((ngx, ngy)),
            pltpu.SemaphoreType.DMA((ngx, ngy)),
        ],
        compiler_params=pltpu.CompilerParams(
            collective_id=0, has_side_effects=True, vmem_limit_bytes=48 * 2**20
        ),
        cost_estimate=pl.CostEstimate(
            flops=60 * basis.size, bytes_accessed=8 * basis.size, transcendentals=0
        ),
    )(basis, reaction)


def write_kernel(nat, tiles, extended, coarse, blocks, out_sem, coarse_sem):
    width, cx, cy, cz = extended.shape
    ngx, ngy = tiles.shape[:2]
    yi = nat.shape[1]

    @pl.loop(0, cx)
    def _(x):
        for y in range(cy):
            pltpu.make_async_copy(
                nat.at[x, y % yi, pl.ds((y // yi) * width, width), :],
                extended.at[:, x, y, :],
                out_sem.at[x],
            ).start()

    nothing = jnp.zeros((width, width), F32)

    @pl.loop(0, ngx)
    def _(row):
        for col in range(ngy):
            s = row * ngy + col
            below, above = jnp.maximum(row - 1, 0), row
            blocks[s, 0] = unpacked(tiles[row, col, 0], width)
            blocks[s, 1] = jnp.where(row > 0, unpacked(tiles[below, col, 2], width), 0.0)
            blocks[s, 2] = jnp.where(row < ngx - 1, unpacked(tiles[above, col, 1], width), 0.0)
            blocks[s, 3] = unpacked(tiles[row, col - 1, 4], width) if col > 0 else nothing
            blocks[s, 4] = unpacked(tiles[row, col, 3], width) if col < ngy - 1 else nothing

    copy = pltpu.make_async_copy(blocks, coarse, coarse_sem)
    copy.start()

    @pl.loop(0, cx)
    def _(x):
        pltpu.make_async_copy(nat.at[x], nat.at[x], out_sem.at[x]).wait()

    copy.wait()


def write(nat, tiles, shape):
    width, cx, cy, cz = shape
    ngx, ngy = tiles.shape[:2]
    vmem = pl.BlockSpec(memory_space=pltpu.VMEM)
    hbm = pl.BlockSpec(memory_space=pltpu.HBM)
    coarse = (ngx * ngy, 5, width, width)
    return pl.pallas_call(
        write_kernel,
        in_specs=[vmem, vmem],
        out_specs=[hbm, hbm],
        out_shape=[jax.ShapeDtypeStruct(shape, F32), jax.ShapeDtypeStruct(coarse, F32)],
        scratch_shapes=[
            pltpu.VMEM(coarse, F32),
            pltpu.SemaphoreType.DMA((cx,)),
            pltpu.SemaphoreType.DMA,
        ],
        compiler_params=pltpu.CompilerParams(vmem_limit_bytes=16 * 2**20),
    )(nat, tiles)


def on_device(basis, reaction):
    nat, tiles = main(basis, reaction)
    extended, coarse = write(nat, tiles, basis.shape)
    return extended, coarse


def solution(mesh):
    placed = (P(None, "gx", "gy", None), P("gx", "gy", None))
    return jax.shard_map(
        on_device,
        mesh=mesh,
        in_specs=placed,
        out_specs=(P(None, "gx", "gy", None), P()),
        check_vma=False,
    )
```

```python
import functools

import jax
import jax.numpy as jnp
from jax import lax
from jax.experimental import pallas as pl
from jax.experimental.pallas import tpu as pltpu
from jax.sharding import PartitionSpec as P

SWEEPS = 4
OMEGA = 0.8
ROWS = 8
LANES = 128
MESH = pl.DeviceIdType.MESH
F32 = jnp.float32
BF16 = jnp.bfloat16


def split(value):
    high = value.astype(BF16)
    low = (value - high.astype(F32)).astype(BF16)
    return high, low


def thirds(value):
    first = value.astype(BF16)
    rest = value - first.astype(F32)
    second = rest.astype(BF16)
    third = (rest - second.astype(F32)).astype(BF16)
    return jnp.concatenate([first, second, third], axis=0)


def block_sum(square, width):
    half = square.shape[0] // 2
    full = square[:half, :half] + square[:half, half:] + square[half:, :half]
    total = full[:width, :width]
    for i in range(width, half, width):
        total = total + full[i:i + width, i:i + width]
    return total


def packed(block):
    rows = block.shape[0] * block.shape[1] // LANES
    return jnp.concatenate(
        [block[i:i + rows] for i in range(0, block.shape[0], rows)], axis=1
    )


def unpacked(tile, width):
    return jnp.concatenate(
        [tile[:, i:i + width] for i in range(0, LANES, width)], axis=0
    )


def main_kernel(
    ngx, ngy, basis, reaction, nat, tiles,
    react, spread, weight, centre, first, second, lefts, rights,
    gram, face_x, face_y, pairs, diag,
    in_sem, react_sem, face_send, face_recv,
    pair_send_y, pair_recv_y, pair_send_x, pair_recv_x,
    diag_send_y, diag_recv_y, diag_send_x, diag_recv_x,
):
    width, cx, cy, cz = basis.shape
    yo = LANES // width
    yi = cy // yo
    group = cx // yo
    halves = cz // LANES
    ztiles = cz // ROWS
    gx, gy = lax.axis_index("gx"), lax.axis_index("gy")

    barrier = pltpu.get_barrier_semaphore()
    for d in range(1, ngy):
        pl.semaphore_signal(barrier, inc=1, device_id=(gx, lax.rem(gy + d, ngy)), device_id_type=MESH)
    for d in range(1, ngx):
        pl.semaphore_signal(barrier, inc=1, device_id=(lax.rem(gx + d, ngx), gy), device_id_type=MESH)

    load = pltpu.make_async_copy(reaction, react, react_sem)
    load.start()

    def bring(x):
        for y in range(cy):
            pltpu.make_async_copy(
                basis.at[:, x, y, :],
                nat.at[x, y % yi, pl.ds((y // yi) * width, width), :],
                in_sem.at[x],
            ).start()

    bring(0)

    def over_x(peer):
        return pltpu.make_async_remote_copy(
            src_ref=nat.at[0], dst_ref=face_x, send_sem=face_send.at[0], recv_sem=face_recv.at[0],
            device_id=(peer, gy), device_id_type=MESH,
        )

    def over_y(x, upper, peer):
        plane, start = (yi - 1, LANES - width) if upper else (0, 0)
        return pltpu.make_async_remote_copy(
            src_ref=nat.at[x, plane, pl.ds(start, width), :],
            dst_ref=face_y.at[x // yo, pl.ds(lax.rem(x, yo) * width, width), :],
            send_sem=face_send.at[1 + upper], recv_sem=face_recv.at[1 + upper],
            device_id=(gx, peer), device_id_type=MESH,
        )

    middle = (group // 2) * yo

    rows = lax.broadcasted_iota(jnp.int32, (cy, yi * LANES), 0)
    cols = lax.broadcasted_iota(jnp.int32, (cy, yi * LANES), 1)
    chosen = rows == (lax.rem(cols, LANES) // width) * yi + cols // LANES
    pick = jnp.where(chosen, 1.0, 0.0).astype(BF16)
    spread[...] = jnp.concatenate([pick, pick, pick], axis=0)

    def expanded(values):
        return lax.dot_general(
            thirds(values), spread[...], (((0,), (0,)), ((), ())), preferred_element_type=F32
        )

    line = lax.broadcasted_iota(jnp.int32, (cy, cz), 0)
    face_row = (line == 0) | (line == cy - 1)
    blank = jnp.zeros((ROWS, LANES), F32)
    load.wait()

    @pl.loop(1, cx)
    def _(x):
        bring(x)
        scaled = jnp.where(face_row, 0.0, OMEGA / (6.0 + react[x]))
        wide = expanded(scaled)
        for j in range(yi):
            weight[x, j] = wide[:, j * LANES:(j + 1) * LANES]
            for buffer in (first, second):
                buffer[x, j, 0:ROWS, :] = blank
                buffer[x, j, cz + ROWS:cz + 2 * ROWS, :] = blank

    for j in range(yi):
        for buffer in (first, second):
            buffer[0, j, 0:ROWS, :] = blank
            buffer[0, j, cz + ROWS:cz + 2 * ROWS, :] = blank
    gram[...] = jnp.zeros_like(gram)

    pl.semaphore_wait(barrier, ngx + ngy - 2)

    lane = lax.broadcasted_iota(jnp.int32, (ROWS, LANES), 1)
    keep = [jnp.full((ROWS, LANES), 1.0 - OMEGA, F32) for _ in range(yi)]
    keep[0] = jnp.where(lane < width, 1.0, keep[0])
    keep[yi - 1] = jnp.where(lane >= LANES - width, 1.0, keep[yi - 1])

    def land(x):
        pltpu.make_async_copy(nat.at[x], nat.at[x], in_sem.at[x]).wait()

        @pl.when((x < middle) & (gy > 0))
        def _():
            over_y(x, 0, gy - 1).start()

        @pl.when((x >= middle) & (gy < ngy - 1))
        def _():
            over_y(x, 1, gy + 1).start()

    def take_in(x, j, h):
        part = nat[x, j, :, h * LANES:(h + 1) * LANES]
        first[x, j, ROWS + h * LANES:ROWS + (h + 1) * LANES, :] = part.T

    squares = [(j, h) for j in range(yi) for h in range(halves)]

    def line_of(ref, x, t, shift=0):
        return [ref[x, j, pl.ds(ROWS + t * ROWS + shift, ROWS), :] for j in range(yi)]

    def forward(values):
        return pltpu.roll(values[0], LANES - width, 1)

    def backward(values):
        return pltpu.roll(values[yi - 1], width, 1)

    def diagonals(here, up):
        inner = [here[j] + up[j + 1] for j in range(yi - 1)]
        return [backward(here) + up[0]] + inner + [here[yi - 1] + forward(up)]

    def finish(source, target, x, t, here, total):
        below, above = line_of(source, x, t, -1), line_of(source, x, t, 1)
        for j in range(yi):
            around = total[j] + (below[j] + above[j])
            target[x, j, pl.ds(ROWS + t * ROWS, ROWS), :] = (
                keep[j] * here[j] + weight[x, j, pl.ds(t * ROWS, ROWS), :] * around
            )

    def sweep_pair(source, target, x, t):
        field = [line_of(source, x + i, t) for i in range(4)]
        for i in range(1, 3):
            down, here, up = field[i - 1:i + 2]
            near = [backward(here)] + here + [forward(here)]
            total = [(down[j] + up[j]) + (near[j] + near[j + 2]) for j in range(yi)]
            finish(source, target, x + i, t, here, total)

    def sweep(source, target):
        @pl.loop(0, ztiles, unroll=2)
        def _(t):
            here = line_of(source, 1, t)
            old = diagonals(line_of(source, 0, t), here)
            for x in range(1, cx - 1):
                up = line_of(source, x + 1, t)
                new = diagonals(here, up)
                total = [old[j + 1] + new[j] for j in range(yi)]
                finish(source, target, x, t, here, total)
                old, here = new, up

    land(0)

    @pl.when(gx > 0)
    def _():
        over_x(gx - 1).start()

    for x in range(4):
        if x:
            land(x)
        for square in squares:
            take_in(x, *square)

    each = ztiles // (2 * len(squares))

    @pl.loop(0, cx - 4, step=2)
    def _(x):
        land(x + 4)
        land(x + 5)
        for i in range(2):
            for n, square in enumerate(squares):
                take_in(x + 4 + i, *square)
                for m in range(each):
                    sweep_pair(first, second, x, (i * len(squares) + n) * each + m)

    for t in range(ztiles):
        sweep_pair(first, second, cx - 4, t)

    @pl.loop(0, ztiles)
    def _(t):
        for x in (0, cx - 1):
            for j, value in enumerate(line_of(first, x, t)):
                second[x, j, pl.ds(ROWS + t * ROWS, ROWS), :] = value

    sweep(second, first)
    sweep(first, second)

    def joined(ref, start=0, stop=None):
        stop = ref.shape[0] if stop is None else stop
        return jnp.concatenate([ref[i] for i in range(start, stop)], axis=1)

    def couple(start, stop):
        return -block_sum(
            lax.dot_general(
                joined(lefts.at[0], start, stop), joined(lefts.at[1], start, stop),
                (((1,), (1,)), ((), ())), preferred_element_type=F32,
            ),
            width,
        )

    def fill(ref, row, column, value):
        size = value.shape[0]
        for h in range(halves):
            high, low = split(value[:, h * LANES:(h + 1) * LANES])
            ref[column * halves + h, row:row + size] = high
            ref[column * halves + h, LANES + row:LANES + row + size] = low

    @pl.when(gx < ngx - 1)
    def _():
        over_x(gx).wait_recv()

    for j in range(yi):
        fill(lefts.at[0], 0, j, nat[cx - 1, j])
        fill(lefts.at[1], 0, j, face_x[j])
    pairs[gx, gy, 0] = packed(couple(0, yi * halves))

    near, far = face_y.at[pl.ds(0, group // 2)], face_y.at[pl.ds(group // 2, group - group // 2)]

    @pl.when(gy < ngy - 1)
    def _():
        pltpu.make_async_copy(near, near, face_recv.at[1]).wait()

    @pl.when(gy > 0)
    def _():
        pltpu.make_async_copy(far, far, face_recv.at[2]).wait()

    for x in range(cx):
        own = nat[x, yi - 1, LANES - width:, :] if x < middle else nat[x, 0, :width, :]
        fill(lefts.at[0 if x < middle else 1], (x % yo) * width, x // yo, own)
    for j in range(group):
        fill(lefts.at[1 if j < group // 2 else 0], 0, j, face_y[j])
    pairs[gx, gy, 1] = packed(couple(0, (group // 2) * halves))
    pairs[gx, gy, 2] = packed(couple((group // 2) * halves, group * halves))

    @pl.when(gx > 0)
    def _():
        over_x(gx).wait_send()

    @pl.when(gy > 0)
    def _():
        pltpu.make_async_copy(near, near, face_send.at[1]).wait()

    @pl.when(gy < ngy - 1)
    def _():
        pltpu.make_async_copy(far, far, face_send.at[2]).wait()

    def to_y(ref, send, recv, owner, peer):
        piece = ref.at[gx, owner]
        return pltpu.make_async_remote_copy(
            src_ref=piece, dst_ref=piece, send_sem=send.at[peer], recv_sem=recv.at[owner],
            device_id=(gx, peer), device_id_type=MESH,
        )

    def to_x(ref, send, recv, row, owner, peer):
        piece = ref.at[row, owner]
        return pltpu.make_async_remote_copy(
            src_ref=piece, dst_ref=piece, send_sem=send.at[peer, owner], recv_sem=recv.at[row, owner],
            device_id=(peer, gy), device_id_type=MESH,
        )

    ys = [lax.rem(gy + d, ngy) for d in range(1, ngy)]
    xs = [lax.rem(gx + d, ngx) for d in range(1, ngx)]

    def gather_start(ref, send_y, recv_y, send_x, recv_x):
        for peer in ys:
            to_y(ref, send_y, recv_y, gy, peer).start()
        for peer in xs:
            to_x(ref, send_x, recv_x, gx, gy, peer).start()

    def gather_pass(ref, send_y, recv_y, send_x, recv_x):
        for owner in ys:
            to_y(ref, send_y, recv_y, owner, owner).wait_recv()
            for peer in xs:
                to_x(ref, send_x, recv_x, gx, owner, peer).start()

    def gather_end(ref, send_y, recv_y, send_x, recv_x):
        for owner in [gy] + ys:
            for row in xs:
                to_x(ref, send_x, recv_x, row, owner, row).wait_recv()
        for peer in ys:
            to_y(ref, send_y, recv_y, gy, peer).wait_send()
        for owner in [gy] + ys:
            for peer in xs:
                to_x(ref, send_x, recv_x, gx, owner, peer).wait_send()

    pair_way = (pairs, pair_send_y, pair_recv_y, pair_send_x, pair_recv_x)
    diag_way = (diag, diag_send_y, diag_recv_y, diag_send_x, diag_recv_x)
    gather_start(*pair_way)

    source, result = second, first

    def applied(x, i, slot, t, last):
        here, above = line_of(result, x, t), line_of(result, x, t, 1)
        up = None if last else line_of(result, x + 1, t)
        edge = jnp.where(lane >= LANES - width, 0.0, forward(here))
        beside = here[1:] + [edge]
        out = []
        for j in range(yi):
            total = beside[j] + above[j]
            if up is not None:
                total = total + up[j]
            out.append(centre[slot + i, j, t * ROWS:(t + 1) * ROWS, :] * here[j] - total)
        return out

    def block(x, slot, sweeping=True, last=False):
        for i in range(2):
            wide = expanded(3.0 + 0.5 * react[x + i])
            for j in range(yi):
                centre[slot + i, j] = wide[:, j * LANES:(j + 1) * LANES]
        for n in range(ztiles // 2):
            if sweeping:
                for t in (2 * n, 2 * n + 1):
                    sweep_pair(source, result, x + 2, t)
            for i in range(2):
                two = [applied(x + i, i, slot, t, last and i == 1) for t in (2 * n, 2 * n + 1)]
                for j in range(yi):
                    at = j * cz + n * 2 * ROWS
                    both = jnp.concatenate([two[0][j], two[1][j]], axis=0)
                    for part, value in enumerate(split(both)):
                        rights[slot + i, part, at:at + 2 * ROWS] = value
            i, (j, h) = n // len(squares), squares[n % len(squares)]
            part = result[x + i, j, ROWS + h * LANES:ROWS + (h + 1) * LANES, :].T
            nat[x + i, j, :, h * LANES:(h + 1) * LANES] = part
            for half, value in enumerate(split(part)):
                lefts[slot + i, j * halves + h, half * LANES:(half + 1) * LANES] = value

    def multiply(slot, fresh=None):
        for i in range(2):
            total = gram[...] + jnp.dot(
                joined(lefts.at[slot + i]), joined(rights.at[slot + i]), preferred_element_type=F32
            )
            gram[...] = total if fresh is None else jnp.where(fresh, 0.0, total)

    for t in range(ztiles):
        sweep_pair(source, result, 0, t)

    steps = (cx - 4) // 4

    @pl.loop(0, steps)
    def _(n):
        @pl.when(n == steps - 1)
        def _():
            gather_pass(*pair_way)

        multiply(2, n == 0)
        block(4 * n, 0)
        multiply(0)
        block(4 * n + 2, 2)

    multiply(2)
    block(cx - 4, 0, sweeping=False)
    multiply(0)
    block(cx - 2, 2, sweeping=False, last=True)
    multiply(2)

    half = block_sum(gram[...], width)
    diag[gx, gy] = packed(half + half.T)
    gather_start(*diag_way)
    gather_pass(*diag_way)
    gather_end(*pair_way)
    tiles[:, :, 1:] = pairs[...]
    gather_end(*diag_way)
    tiles[:, :, 0] = diag[...]


def main(basis, reaction):
    ngx, ngy = lax.axis_size("gx"), lax.axis_size("gy")
    width, cx, cy, cz = basis.shape
    yo = LANES // width
    yi = cy // yo
    hbm = pl.BlockSpec(memory_space=pltpu.HBM)
    vmem = pl.BlockSpec(memory_space=pltpu.VMEM)
    field = pltpu.VMEM((cx, yi, cz + 2 * ROWS, LANES), F32)
    tile = (width * width // LANES, LANES)
    one, grid = pltpu.SemaphoreType.DMA((ngy,)), pltpu.SemaphoreType.DMA((ngx, ngy))
    return pl.pallas_call(
        functools.partial(main_kernel, ngx, ngy),
        in_specs=[hbm, hbm],
        out_specs=[vmem, vmem],
        out_shape=[
            jax.ShapeDtypeStruct((cx, yi, LANES, cz), F32),
            jax.ShapeDtypeStruct((ngx, ngy, 4) + tile, F32),
        ],
        scratch_shapes=[
            pltpu.VMEM((cx, cy, cz), F32),
            pltpu.VMEM((3 * cy, yi * LANES), BF16),
            pltpu.VMEM((cx, yi, cz, LANES), F32),
            pltpu.VMEM((4, yi, cz, LANES), F32),
            field, field,
            pltpu.VMEM((4, yi * cz // LANES, 2 * LANES, LANES), BF16),
            pltpu.VMEM((4, 2, yi * cz, LANES), BF16),
            pltpu.VMEM((2 * LANES, 2 * LANES), F32),
            pltpu.VMEM((yi, LANES, cz), F32),
            pltpu.VMEM((cx // yo, LANES, cz), F32),
            pltpu.VMEM((ngx, ngy, 3) + tile, F32),
            pltpu.VMEM((ngx, ngy) + tile, F32),
            pltpu.SemaphoreType.DMA((cx,)),
            pltpu.SemaphoreType.DMA,
            pltpu.SemaphoreType.DMA((3,)),
            pltpu.SemaphoreType.DMA((3,)),
            one, one, grid, grid, one, one, grid, grid,
        ],
        compiler_params=pltpu.CompilerParams(
            collective_id=0, has_side_effects=True, vmem_limit_bytes=40 * 2**20
        ),
        cost_estimate=pl.CostEstimate(
            flops=60 * basis.size, bytes_accessed=8 * basis.size, transcendentals=0
        ),
    )(basis, reaction)


def write_kernel(nat, tiles, extended, coarse, blocks, out_sem, coarse_sem):
    width, cx, cy, cz = extended.shape
    ngx, ngy = tiles.shape[:2]
    yi = nat.shape[1]

    @pl.loop(0, cx)
    def _(x):
        for y in range(cy):
            pltpu.make_async_copy(
                nat.at[x, y % yi, pl.ds((y // yi) * width, width), :],
                extended.at[:, x, y, :],
                out_sem.at[x],
            ).start()

    nothing = jnp.zeros((width, width), F32)

    @pl.loop(0, ngx)
    def _(row):
        for col in range(ngy):
            s = row * ngy + col
            below = jnp.maximum(row - 1, 0)
            blocks[s, 0] = unpacked(tiles[row, col, 0], width)
            lower = unpacked(tiles[below, col, 1], width).T
            blocks[s, 1] = jnp.where(row > 0, lower, 0.0)
            blocks[s, 2] = jnp.where(row < ngx - 1, unpacked(tiles[row, col, 1], width), 0.0)
            blocks[s, 3] = nothing
            if col > 0:
                blocks[s, 3] = unpacked(tiles[row, col - 1, 2] + tiles[row, col, 3], width).T
            blocks[s, 4] = nothing
            if col < ngy - 1:
                blocks[s, 4] = unpacked(tiles[row, col, 2] + tiles[row, col + 1, 3], width)

    copy = pltpu.make_async_copy(blocks, coarse, coarse_sem)
    copy.start()

    @pl.loop(0, cx)
    def _(x):
        pltpu.make_async_copy(nat.at[x], nat.at[x], out_sem.at[x]).wait()

    copy.wait()


def write(nat, tiles, shape):
    width, cx, cy, cz = shape
    ngx, ngy = tiles.shape[:2]
    vmem = pl.BlockSpec(memory_space=pltpu.VMEM)
    hbm = pl.BlockSpec(memory_space=pltpu.HBM)
    coarse = (ngx * ngy, 5, width, width)
    return pl.pallas_call(
        write_kernel,
        in_specs=[vmem, vmem],
        out_specs=[hbm, hbm],
        out_shape=[jax.ShapeDtypeStruct(shape, F32), jax.ShapeDtypeStruct(coarse, F32)],
        scratch_shapes=[
            pltpu.VMEM(coarse, F32),
            pltpu.SemaphoreType.DMA((cx,)),
            pltpu.SemaphoreType.DMA,
        ],
        compiler_params=pltpu.CompilerParams(vmem_limit_bytes=16 * 2**20),
    )(nat, tiles)


def on_device(basis, reaction):
    nat, tiles = main(basis, reaction)
    extended, coarse = write(nat, tiles, basis.shape)
    return extended, coarse


def solution(mesh):
    placed = (P(None, "gx", "gy", None), P("gx", "gy", None))
    return jax.shard_map(
        on_device,
        mesh=mesh,
        in_specs=placed,
        out_specs=(P(None, "gx", "gy", None), P()),
        check_vma=False,
    )
```

```python
import functools

import jax
import jax.numpy as jnp
from jax import lax
from jax.experimental import pallas as pl
from jax.experimental.pallas import tpu as pltpu
from jax.sharding import PartitionSpec as P

SWEEPS = 4
OMEGA = 0.8
ROWS = 8
LANES = 128
MESH = pl.DeviceIdType.MESH
F32 = jnp.float32
BF16 = jnp.bfloat16


def split(value):
    high = value.astype(BF16)
    low = (value - high.astype(F32)).astype(BF16)
    return high, low


def thirds(value):
    first = value.astype(BF16)
    rest = value - first.astype(F32)
    second = rest.astype(BF16)
    third = (rest - second.astype(F32)).astype(BF16)
    return jnp.concatenate([first, second, third], axis=0)


def combined(wide):
    half = wide.shape[0] // 2
    return wide[:half, :half] + wide[:half, half:] + wide[half:, :half]


def block_sum(wide, width):
    full = combined(wide)
    total = full[:width, :width]
    for i in range(width, full.shape[0], width):
        total = total + full[i:i + width, i:i + width]
    return total


def packed(block):
    rows = block.shape[0] * block.shape[1] // LANES
    return jnp.concatenate(
        [block[i:i + rows] for i in range(0, block.shape[0], rows)], axis=1
    )


def unpacked(tile, width):
    return jnp.concatenate(
        [tile[:, i:i + width] for i in range(0, LANES, width)], axis=0
    )


def main_kernel(
    ngx, ngy, basis, reaction, nat, pairs_out, diag_out,
    react, spread, weight, centre, first, second, lefts, rights,
    gram, square, face_x, face_y, pairs, diag,
    in_sem, react_sem, face_send, face_recv, pair_sem, diag_sem,
):
    width, cx, cy, cz = basis.shape
    yo = LANES // width
    yi = cy // yo
    group = cx // yo
    halves = cz // LANES
    ztiles = cz // ROWS
    gx, gy = lax.axis_index("gx"), lax.axis_index("gy")

    lines = nat.reshape(cx, halves, width * cy, LANES)
    count = ngx * ngy
    me = gx * ngy + gy

    def other(d):
        peer = lax.rem(me + d, count)
        return (peer // ngy, lax.rem(peer, ngy))

    barrier = pltpu.get_barrier_semaphore()

    @pl.loop(1, count)
    def _(d):
        pl.semaphore_signal(barrier, inc=1, device_id=other(d), device_id_type=MESH)

    load = pltpu.make_async_copy(reaction, react, react_sem)
    load.start()

    @pl.loop(0, cx)
    def _(x):
        for h in range(halves):
            pltpu.make_async_copy(
                basis.at[:, x, :, h * LANES:(h + 1) * LANES], nat.at[x, h], in_sem.at[x]
            ).start()

    def over_x(peer):
        return pltpu.make_async_remote_copy(
            src_ref=nat.at[0], dst_ref=face_x, send_sem=face_send.at[0], recv_sem=face_recv.at[0],
            device_id=(peer, gy), device_id_type=MESH,
        )

    def over_y(x, upper, peer):
        return pltpu.make_async_remote_copy(
            src_ref=nat.at[x, :, :, cy - 1 if upper else 0, :],
            dst_ref=face_y.at[x // yo, :, pl.ds(lax.rem(x, yo) * width, width), :],
            send_sem=face_send.at[1 + upper], recv_sem=face_recv.at[1 + upper],
            device_id=(gx, peer), device_id_type=MESH,
        )

    middle = (group // 2) * yo

    rows = lax.broadcasted_iota(jnp.int32, (cy, yi * LANES), 0)
    cols = lax.broadcasted_iota(jnp.int32, (cy, yi * LANES), 1)
    chosen = rows == lax.rem(cols, yo) * yi + cols // LANES
    pick = jnp.where(chosen, 1.0, 0.0).astype(BF16)
    spread[...] = jnp.concatenate([pick, pick, pick], axis=0)

    def expanded(values):
        return lax.dot_general(
            thirds(values), spread[...], (((0,), (0,)), ((), ())), preferred_element_type=F32
        )

    line = lax.broadcasted_iota(jnp.int32, (cy, cz), 0)
    face_row = (line == 0) | (line == cy - 1)
    blank = jnp.zeros((ROWS, LANES), F32)
    load.wait()

    def weigh(x):
        wide = expanded(jnp.where(face_row, 0.0, OMEGA / (6.0 + react[x])))
        for j in range(yi):
            weight[x, j] = wide[:, j * LANES:(j + 1) * LANES]

    for x in (1, 2):
        weigh(x)

    @pl.loop(0, cx)
    def _(x):
        for j in range(yi):
            for buffer in (first, second):
                buffer[x, j, 0:ROWS, :] = blank
                buffer[x, j, cz + ROWS:cz + 2 * ROWS, :] = blank

    gram[...] = jnp.zeros_like(gram)

    pl.semaphore_wait(barrier, count - 1)

    lane = lax.broadcasted_iota(jnp.int32, (ROWS, LANES), 1)
    keep = [jnp.full((ROWS, LANES), 1.0 - OMEGA, F32) for _ in range(yi)]
    upper_lane = lax.rem(lane, yo) == yo - 1
    keep[0] = jnp.where(lax.rem(lane, yo) == 0, 1.0, keep[0])
    keep[yi - 1] = jnp.where(upper_lane, 1.0, keep[yi - 1])

    def land(x):
        pltpu.make_async_copy(nat.at[x], nat.at[x], in_sem.at[x]).wait()

        @pl.when((x < middle) & (gy > 0))
        def _():
            over_y(x, 0, gy - 1).start()

        @pl.when((x >= middle) & (gy < ngy - 1))
        def _():
            over_y(x, 1, gy + 1).start()

    def take_in(x, j, h):
        part = lines[x, h, pl.ds(j, LANES, stride=yi), :]
        first[x, j, ROWS + h * LANES:ROWS + (h + 1) * LANES, :] = part.T

    squares = [(j, h) for j in range(yi) for h in range(halves)]

    def line_of(ref, x, t, shift=0):
        return [ref[x, j, pl.ds(ROWS + t * ROWS + shift, ROWS), :] for j in range(yi)]

    def forward(values):
        return pltpu.roll(values[0], LANES - 1, 1)

    def backward(values):
        return pltpu.roll(values[yi - 1], 1, 1)

    def diagonals(here, up):
        inner = [here[j] + up[j + 1] for j in range(yi - 1)]
        return [backward(here) + up[0]] + inner + [here[yi - 1] + forward(up)]

    def finish(source, target, x, t, here, total):
        below, above = line_of(source, x, t, -1), line_of(source, x, t, 1)
        for j in range(yi):
            around = total[j] + (below[j] + above[j])
            target[x, j, pl.ds(ROWS + t * ROWS, ROWS), :] = (
                keep[j] * here[j] + weight[x, j, pl.ds(t * ROWS, ROWS), :] * around
            )

    def sweep_pair(source, target, x, t):
        field = [line_of(source, x + i, t) for i in range(4)]
        for i in range(1, 3):
            down, here, up = field[i - 1:i + 2]
            near = [backward(here)] + here + [forward(here)]
            total = [(down[j] + up[j]) + (near[j] + near[j + 2]) for j in range(yi)]
            finish(source, target, x + i, t, here, total)

    def sweep(source, target):
        @pl.loop(0, ztiles, unroll=2)
        def _(t):
            here = line_of(source, 1, t)
            old = diagonals(line_of(source, 0, t), here)
            for x in range(1, cx - 1):
                up = line_of(source, x + 1, t)
                new = diagonals(here, up)
                total = [old[j + 1] + new[j] for j in range(yi)]
                finish(source, target, x, t, here, total)
                old, here = new, up

    land(0)

    @pl.when(gx > 0)
    def _():
        over_x(gx - 1).start()

    for x in range(4):
        if x:
            land(x)
        for at in squares:
            take_in(x, *at)

    each = ztiles // (2 * len(squares))

    @pl.loop(0, cx - 4, step=2)
    def _(x):
        land(x + 4)
        land(x + 5)
        weigh(x + 3)
        weigh(x + 4)
        for i in range(2):
            for n, at in enumerate(squares):
                take_in(x + 4 + i, *at)
                for m in range(each):
                    sweep_pair(first, second, x, (i * len(squares) + n) * each + m)

    for t in range(ztiles):
        sweep_pair(first, second, cx - 4, t)

    @pl.loop(0, ztiles)
    def _(t):
        for x in (0, cx - 1):
            for j, value in enumerate(line_of(first, x, t)):
                second[x, j, pl.ds(ROWS + t * ROWS, ROWS), :] = value

    sweep(second, first)
    sweep(first, second)

    def joined(ref, start=0, stop=None):
        stop = ref.shape[0] if stop is None else stop
        return jnp.concatenate([ref[i] for i in range(start, stop)], axis=1)

    def couple(start, stop):
        return lax.dot_general(
            joined(lefts.at[0], start, stop), joined(lefts.at[1], start, stop),
            (((1,), (1,)), ((), ())), preferred_element_type=F32,
        )

    def strided_sum(wide):
        square[...] = combined(wide)
        turned = jnp.concatenate(
            [square[pl.ds(g, width, stride=yo), :] for g in range(yo)], axis=0
        ).T
        square[...] = turned
        total = square[pl.ds(0, width, stride=yo), :][:, :width]
        for g in range(1, yo):
            total = total + square[pl.ds(g, width, stride=yo), :][:, g * width:(g + 1) * width]
        return total

    def fill(ref, row, column, value):
        size = value.shape[0]
        for half, part in enumerate(split(value)):
            ref[column, half * LANES + row:half * LANES + row + size] = part

    @pl.when(gx < ngx - 1)
    def _():
        over_x(gx).wait_recv()

    for n, (j, h) in enumerate(squares):
        fill(lefts.at[0], 0, n, face_x.reshape(halves, width * cy, LANES)[h, pl.ds(j, LANES, stride=yi), :])
        fill(lefts.at[1], 0, n, lines[cx - 1, h, pl.ds(j, LANES, stride=yi), :])
    pairs[gx, gy, 0] = packed(-strided_sum(couple(0, len(squares))))

    near, far = face_y.at[pl.ds(0, group // 2)], face_y.at[pl.ds(group // 2, group - group // 2)]

    @pl.when(gy < ngy - 1)
    def _():
        pltpu.make_async_copy(near, near, face_recv.at[1]).wait()

    @pl.when(gy > 0)
    def _():
        pltpu.make_async_copy(far, far, face_recv.at[2]).wait()

    for x in range(cx):
        for h in range(halves):
            own = lines[x, h, pl.ds(cy - 1 if x < middle else 0, width, stride=cy), :]
            at = (x // yo) * halves + h
            fill(lefts.at[0 if x < middle else 1], (x % yo) * width, at, own)
    cut = (group // 2) * halves
    for c in range(group):
        for h in range(halves):
            at = c * halves + h
            fill(lefts.at[1 if at < cut else 0], 0, at, face_y[c, h])
    pairs[gx, gy, 1] = packed(-block_sum(couple(0, cut), width))
    pairs[gx, gy, 2] = packed(-block_sum(couple(cut, group * halves), width))

    @pl.when(gx > 0)
    def _():
        over_x(gx).wait_send()

    @pl.when(gy > 0)
    def _():
        pltpu.make_async_copy(near, near, face_send.at[1]).wait()

    @pl.when(gy < ngy - 1)
    def _():
        pltpu.make_async_copy(far, far, face_send.at[2]).wait()

    def to_y(peer):
        piece = pairs.at[gx, gy]
        return pltpu.make_async_remote_copy(
            src_ref=piece, dst_ref=piece, send_sem=pair_sem.at[0], recv_sem=pair_sem.at[1],
            device_id=(gx, peer), device_id_type=MESH,
        )

    def to_x(peer):
        piece = pairs.at[gx]
        return pltpu.make_async_remote_copy(
            src_ref=piece, dst_ref=piece, send_sem=pair_sem.at[2], recv_sem=pair_sem.at[3],
            device_id=(peer, gy), device_id_type=MESH,
        )

    def to_all(d):
        piece = diag.at[me]
        return pltpu.make_async_remote_copy(
            src_ref=piece, dst_ref=piece, send_sem=diag_sem.at[0], recv_sem=diag_sem.at[1],
            device_id=other(d), device_id_type=MESH,
        )

    def await_bytes(ref, sem):
        pltpu.make_async_copy(ref, ref, sem).wait()

    row_rest, grid_rest = pairs.at[0, pl.ds(0, ngy - 1)], pairs.at[pl.ds(0, ngx - 1)]
    for d in range(1, ngy):
        to_y(lax.rem(gy + d, ngy)).start()

    source, result = second, first

    def applied(x, i, slot, t, last):
        here, above = line_of(result, x, t), line_of(result, x, t, 1)
        up = None if last else line_of(result, x + 1, t)
        edge = jnp.where(upper_lane, 0.0, forward(here))
        beside = here[1:] + [edge]
        out = []
        for j in range(yi):
            total = beside[j] + above[j]
            if up is not None:
                total = total + up[j]
            out.append(centre[slot + i, j, t * ROWS:(t + 1) * ROWS, :] * here[j] - total)
        return out

    def block(x, slot, sweeping=True, last=False):
        for i in range(2):
            wide = expanded(3.0 + 0.5 * react[x + i])
            for j in range(yi):
                centre[slot + i, j] = wide[:, j * LANES:(j + 1) * LANES]
        for n in range(ztiles // 2):
            if sweeping:
                for t in (2 * n, 2 * n + 1):
                    sweep_pair(source, result, x + 2, t)
            for i in range(2):
                two = [applied(x + i, i, slot, t, last and i == 1) for t in (2 * n, 2 * n + 1)]
                for j in range(yi):
                    at = j * cz + n * 2 * ROWS
                    both = jnp.concatenate([two[0][j], two[1][j]], axis=0)
                    for part, value in enumerate(split(both)):
                        rights[slot + i, part, at:at + 2 * ROWS] = value
            i, (j, h) = n // len(squares), squares[n % len(squares)]
            part = result[x + i, j, ROWS + h * LANES:ROWS + (h + 1) * LANES, :].T
            lines[x + i, h, pl.ds(j, LANES, stride=yi), :] = part
            for half, value in enumerate(split(part)):
                lefts[slot + i, j * halves + h, half * LANES:(half + 1) * LANES] = value

    def multiply(slot, fresh=None):
        for i in range(2):
            total = gram[...] + jnp.dot(
                joined(lefts.at[slot + i]), joined(rights.at[slot + i]), preferred_element_type=F32
            )
            gram[...] = total if fresh is None else jnp.where(fresh, 0.0, total)

    for t in range(ztiles):
        sweep_pair(source, result, 0, t)

    steps = (cx - 4) // 4

    @pl.loop(0, steps)
    def _(n):
        @pl.when(n == steps - 1)
        def _():
            await_bytes(row_rest, pair_sem.at[1])
            for d in range(1, ngx):
                to_x(lax.rem(gx + d, ngx)).start()

        multiply(2, n == 0)
        block(4 * n, 0)
        multiply(0)
        block(4 * n + 2, 2)

    multiply(2)
    block(cx - 4, 0, sweeping=False)
    multiply(0)
    block(cx - 2, 2, sweeping=False, last=True)
    multiply(2)

    half = strided_sum(gram[...])
    diag[me] = packed(half + half.T)

    @pl.loop(1, count)
    def _(d):
        to_all(d).start()

    await_bytes(row_rest, pair_sem.at[0])
    await_bytes(grid_rest, pair_sem.at[3])
    await_bytes(grid_rest, pair_sem.at[2])
    pairs_out[...] = pairs[...]
    all_rest = diag.at[pl.ds(0, count - 1)]
    await_bytes(all_rest, diag_sem.at[1])
    await_bytes(all_rest, diag_sem.at[0])
    diag_out[...] = diag[...]


def main(basis, reaction):
    ngx, ngy = lax.axis_size("gx"), lax.axis_size("gy")
    width, cx, cy, cz = basis.shape
    yo = LANES // width
    yi = cy // yo
    hbm = pl.BlockSpec(memory_space=pltpu.HBM)
    vmem = pl.BlockSpec(memory_space=pltpu.VMEM)
    field = pltpu.VMEM((cx, yi, cz + 2 * ROWS, LANES), F32)
    tile = (width * width // LANES, LANES)
    return pl.pallas_call(
        functools.partial(main_kernel, ngx, ngy),
        in_specs=[hbm, hbm],
        out_specs=[vmem, vmem, vmem],
        out_shape=[
            jax.ShapeDtypeStruct((cx, cz // LANES, width, cy, LANES), F32),
            jax.ShapeDtypeStruct((ngx, ngy, 3) + tile, F32),
            jax.ShapeDtypeStruct((ngx * ngy,) + tile, F32),
        ],
        scratch_shapes=[
            pltpu.VMEM((cx, cy, cz), F32),
            pltpu.VMEM((3 * cy, yi * LANES), BF16),
            pltpu.VMEM((cx, yi, cz, LANES), F32),
            pltpu.VMEM((4, yi, cz, LANES), F32),
            field, field,
            pltpu.VMEM((4, yi * cz // LANES, 2 * LANES, LANES), BF16),
            pltpu.VMEM((4, 2, yi * cz, LANES), BF16),
            pltpu.VMEM((2 * LANES, 2 * LANES), F32),
            pltpu.VMEM((LANES, LANES), F32),
            pltpu.VMEM((cz // LANES, width, cy, LANES), F32),
            pltpu.VMEM((cx // yo, cz // LANES, LANES, LANES), F32),
            pltpu.VMEM((ngx, ngy, 3) + tile, F32),
            pltpu.VMEM((ngx * ngy,) + tile, F32),
            pltpu.SemaphoreType.DMA((cx,)),
            pltpu.SemaphoreType.DMA,
            pltpu.SemaphoreType.DMA((3,)),
            pltpu.SemaphoreType.DMA((3,)),
            pltpu.SemaphoreType.DMA((4,)),
            pltpu.SemaphoreType.DMA((2,)),
        ],
        compiler_params=pltpu.CompilerParams(
            collective_id=0, has_side_effects=True, vmem_limit_bytes=40 * 2**20
        ),
        cost_estimate=pl.CostEstimate(
            flops=60 * basis.size, bytes_accessed=8 * basis.size, transcendentals=0
        ),
    )(basis, reaction)


def write_kernel(nat, pairs, diag, extended, coarse, blocks, out_sem, coarse_sem):
    width, cx, cy, cz = extended.shape
    ngx, ngy = pairs.shape[:2]

    @pl.loop(0, cx)
    def _(x):
        for h in range(cz // LANES):
            pltpu.make_async_copy(
                nat.at[x, h], extended.at[:, x, :, h * LANES:(h + 1) * LANES], out_sem
            ).start()

    nothing = jnp.zeros((width, width), F32)

    @pl.loop(0, ngx)
    def _(row):
        for col in range(ngy):
            s = row * ngy + col
            below = jnp.maximum(row - 1, 0)
            blocks[s, 0] = unpacked(diag[s], width)
            lower = unpacked(pairs[below, col, 0], width).T
            blocks[s, 1] = jnp.where(row > 0, lower, 0.0)
            blocks[s, 2] = jnp.where(row < ngx - 1, unpacked(pairs[row, col, 0], width), 0.0)
            blocks[s, 3] = nothing
            if col > 0:
                blocks[s, 3] = unpacked(pairs[row, col - 1, 1] + pairs[row, col, 2], width).T
            blocks[s, 4] = nothing
            if col < ngy - 1:
                blocks[s, 4] = unpacked(pairs[row, col, 1] + pairs[row, col + 1, 2], width)

    copy = pltpu.make_async_copy(blocks, coarse, coarse_sem)
    copy.start()
    pltpu.make_async_copy(nat, nat, out_sem).wait()
    copy.wait()


def write(nat, pairs, diag, shape):
    width = shape[0]
    vmem = pl.BlockSpec(memory_space=pltpu.VMEM)
    hbm = pl.BlockSpec(memory_space=pltpu.HBM)
    coarse = (diag.shape[0], 5, width, width)
    return pl.pallas_call(
        write_kernel,
        in_specs=[vmem, vmem, vmem],
        out_specs=[hbm, hbm],
        out_shape=[jax.ShapeDtypeStruct(shape, F32), jax.ShapeDtypeStruct(coarse, F32)],
        scratch_shapes=[
            pltpu.VMEM(coarse, F32),
            pltpu.SemaphoreType.DMA,
            pltpu.SemaphoreType.DMA,
        ],
        compiler_params=pltpu.CompilerParams(vmem_limit_bytes=16 * 2**20),
    )(nat, pairs, diag)


def on_device(basis, reaction):
    return write(*main(basis, reaction), basis.shape)


def solution(mesh):
    placed = (P(None, "gx", "gy", None), P("gx", "gy", None))
    return jax.shard_map(
        on_device,
        mesh=mesh,
        in_specs=placed,
        out_specs=(P(None, "gx", "gy", None), P()),
        check_vma=False,
    )
```

```python
import functools

import jax
import jax.numpy as jnp
from jax import lax
from jax.experimental import pallas as pl
from jax.experimental.pallas import tpu as pltpu
from jax.sharding import PartitionSpec as P

SWEEPS = 4
OMEGA = 0.8
ROWS = 8
LANES = 128
MESH = pl.DeviceIdType.MESH
F32 = jnp.float32
BF16 = jnp.bfloat16


def split(value):
    high = value.astype(BF16)
    low = (value - high.astype(F32)).astype(BF16)
    return high, low


def thirds(value):
    first = value.astype(BF16)
    rest = value - first.astype(F32)
    second = rest.astype(BF16)
    third = (rest - second.astype(F32)).astype(BF16)
    return jnp.concatenate([first, second, third], axis=0)


def combined(wide):
    half = wide.shape[0] // 2
    return wide[:half, :half] + wide[:half, half:] + wide[half:, :half]


def block_sum(wide, width):
    full = combined(wide)
    total = full[:width, :width]
    for i in range(width, full.shape[0], width):
        total = total + full[i:i + width, i:i + width]
    return total


def packed(block):
    rows = block.shape[0] * block.shape[1] // LANES
    return jnp.concatenate(
        [block[i:i + rows] for i in range(0, block.shape[0], rows)], axis=1
    )


def unpacked(tile, width):
    return jnp.concatenate(
        [tile[:, i:i + width] for i in range(0, LANES, width)], axis=0
    )


def main_kernel(
    ngx, ngy, basis, reaction, nat, pairs_out, diag_out,
    react, spread, weight, centre, first, second, lefts, rights,
    gram, square, face_x, face_y, pairs, diag,
    in_sem, react_sem, face_send, face_recv, pair_sem, diag_sem,
):
    width, cx, cy, cz = basis.shape
    yo = LANES // width
    yi = cy // yo
    group = cx // yo
    halves = cz // LANES
    ztiles = cz // ROWS
    gx, gy = lax.axis_index("gx"), lax.axis_index("gy")

    lines = nat.reshape(cx, halves, width * cy, LANES)
    count = ngx * ngy
    me = gx * ngy + gy

    def other(d):
        peer = lax.rem(me + d, count)
        return (peer // ngy, lax.rem(peer, ngy))

    barrier = pltpu.get_barrier_semaphore()

    @pl.loop(1, count)
    def _(d):
        pl.semaphore_signal(barrier, inc=1, device_id=other(d), device_id_type=MESH)

    load = pltpu.make_async_copy(reaction, react, react_sem)
    load.start()

    @pl.loop(0, cx)
    def _(x):
        for h in range(halves):
            pltpu.make_async_copy(
                basis.at[:, x, :, h * LANES:(h + 1) * LANES], nat.at[x, h], in_sem.at[x]
            ).start()

    def over_x(peer):
        return pltpu.make_async_remote_copy(
            src_ref=nat.at[0], dst_ref=face_x, send_sem=face_send.at[0], recv_sem=face_recv.at[0],
            device_id=(peer, gy), device_id_type=MESH,
        )

    def over_y(x, upper, peer):
        return pltpu.make_async_remote_copy(
            src_ref=nat.at[x, :, :, cy - 1 if upper else 0, :],
            dst_ref=face_y.at[x // yo, :, pl.ds(lax.rem(x, yo) * width, width), :],
            send_sem=face_send.at[1 + upper], recv_sem=face_recv.at[1 + upper],
            device_id=(gx, peer), device_id_type=MESH,
        )

    middle = (group // 2) * yo

    rows = lax.broadcasted_iota(jnp.int32, (cy, yi * LANES), 0)
    cols = lax.broadcasted_iota(jnp.int32, (cy, yi * LANES), 1)
    chosen = rows == lax.rem(cols, yo) * yi + cols // LANES
    pick = jnp.where(chosen, 1.0, 0.0).astype(BF16)
    spread[...] = jnp.concatenate([pick, pick, pick], axis=0)

    def expanded(values):
        return lax.dot_general(
            thirds(values), spread[...], (((0,), (0,)), ((), ())), preferred_element_type=F32
        )

    line = lax.broadcasted_iota(jnp.int32, (cy, cz), 0)
    face_row = (line == 0) | (line == cy - 1)
    blank = jnp.zeros((ROWS, LANES), F32)
    load.wait()

    def weigh(x):
        wide = expanded(jnp.where(face_row, 0.0, OMEGA / (6.0 + react[x])))
        for j in range(yi):
            weight[x, j] = wide[:, j * LANES:(j + 1) * LANES]

    for x in (1, 2):
        weigh(x)

    @pl.loop(0, ztiles + 2)
    def _(t):
        for j in range(yi):
            first[cx, j, pl.ds(t * ROWS, ROWS), :] = blank

    @pl.loop(0, cx)
    def _(x):
        for j in range(yi):
            for buffer in (first, second):
                buffer[x, j, 0:ROWS, :] = blank
                buffer[x, j, cz + ROWS:cz + 2 * ROWS, :] = blank

    gram[...] = jnp.zeros_like(gram)

    lane = lax.broadcasted_iota(jnp.int32, (ROWS, LANES), 1)
    keep = [jnp.full((ROWS, LANES), 1.0 - OMEGA, F32) for _ in range(yi)]
    upper_lane = lax.rem(lane, yo) == yo - 1
    keep[0] = jnp.where(lax.rem(lane, yo) == 0, 1.0, keep[0])
    keep[yi - 1] = jnp.where(upper_lane, 1.0, keep[yi - 1])

    def land(x):
        pltpu.make_async_copy(nat.at[x], nat.at[x], in_sem.at[x]).wait()

    def take_in(x, j, h):
        part = lines[x, h, pl.ds(j, LANES, stride=yi), :]
        first[x, j, ROWS + h * LANES:ROWS + (h + 1) * LANES, :] = part.T

    squares = [(j, h) for j in range(yi) for h in range(halves)]

    def line_of(ref, x, t, shift=0):
        return [ref[x, j, pl.ds(ROWS + t * ROWS + shift, ROWS), :] for j in range(yi)]

    def forward(values):
        return pltpu.roll(values[0], LANES - 1, 1)

    def backward(values):
        return pltpu.roll(values[yi - 1], 1, 1)

    def diagonals(here, up):
        inner = [here[j] + up[j + 1] for j in range(yi - 1)]
        return [backward(here) + up[0]] + inner + [here[yi - 1] + forward(up)]

    def finish(source, target, x, t, here, total):
        below, above = line_of(source, x, t, -1), line_of(source, x, t, 1)
        for j in range(yi):
            around = total[j] + (below[j] + above[j])
            target[x, j, pl.ds(ROWS + t * ROWS, ROWS), :] = (
                keep[j] * here[j] + weight[x, j, pl.ds(t * ROWS, ROWS), :] * around
            )

    def sweep_pair(source, target, x, t):
        field = [line_of(source, x + i, t) for i in range(4)]
        for i in range(1, 3):
            down, here, up = field[i - 1:i + 2]
            near = [backward(here)] + here + [forward(here)]
            total = [(down[j] + up[j]) + (near[j] + near[j + 2]) for j in range(yi)]
            finish(source, target, x + i, t, here, total)

    def sweep(source, target):
        @pl.loop(0, ztiles, unroll=2)
        def _(t):
            here = line_of(source, 1, t)
            old = diagonals(line_of(source, 0, t), here)
            for x in range(1, cx - 1):
                up = line_of(source, x + 1, t)
                new = diagonals(here, up)
                total = [old[j + 1] + new[j] for j in range(yi)]
                finish(source, target, x, t, here, total)
                old, here = new, up

    for x in range(4):
        land(x)
        for at in squares:
            take_in(x, *at)

    each = ztiles // (2 * len(squares))

    @pl.loop(0, cx - 4, step=2)
    def _(x):
        land(x + 4)
        land(x + 5)
        weigh(x + 3)
        weigh(x + 4)
        for i in range(2):
            for n, at in enumerate(squares):
                take_in(x + 4 + i, *at)
                for m in range(each):
                    sweep_pair(first, second, x, (i * len(squares) + n) * each + m)

    pl.semaphore_wait(barrier, count - 1)

    @pl.when(gx > 0)
    def _():
        over_x(gx - 1).start()

    @pl.when(gy > 0)
    def _():
        @pl.loop(0, middle)
        def _(x):
            over_y(x, 0, gy - 1).start()

    @pl.when(gy < ngy - 1)
    def _():
        @pl.loop(middle, cx)
        def _(x):
            over_y(x, 1, gy + 1).start()

    for t in range(ztiles):
        sweep_pair(first, second, cx - 4, t)

    @pl.loop(0, ztiles)
    def _(t):
        for x in (0, cx - 1):
            for j, value in enumerate(line_of(first, x, t)):
                second[x, j, pl.ds(ROWS + t * ROWS, ROWS), :] = value

    sweep(second, first)
    sweep(first, second)
    sweep(second, first)

    def joined(ref, start=0, stop=None):
        stop = ref.shape[0] if stop is None else stop
        return jnp.concatenate([ref[i] for i in range(start, stop)], axis=1)

    def couple(start, stop):
        return lax.dot_general(
            joined(lefts.at[0], start, stop), joined(lefts.at[1], start, stop),
            (((1,), (1,)), ((), ())), preferred_element_type=F32,
        )

    def strided_sum(wide):
        square[...] = combined(wide)
        turned = jnp.concatenate(
            [square[pl.ds(g, width, stride=yo), :] for g in range(yo)], axis=0
        ).T
        square[...] = turned
        total = square[pl.ds(0, width, stride=yo), :][:, :width]
        for g in range(1, yo):
            total = total + square[pl.ds(g, width, stride=yo), :][:, g * width:(g + 1) * width]
        return total

    def fill(ref, row, column, value):
        size = value.shape[0]
        for half, part in enumerate(split(value)):
            ref[column, half * LANES + row:half * LANES + row + size] = part

    @pl.when(gx < ngx - 1)
    def _():
        over_x(gx).wait_recv()

    for n, (j, h) in enumerate(squares):
        fill(lefts.at[0], 0, n, face_x.reshape(halves, width * cy, LANES)[h, pl.ds(j, LANES, stride=yi), :])
        fill(lefts.at[1], 0, n, lines[cx - 1, h, pl.ds(j, LANES, stride=yi), :])
    pairs[gx, gy, 0] = packed(-strided_sum(couple(0, len(squares))))

    near, far = face_y.at[pl.ds(0, group // 2)], face_y.at[pl.ds(group // 2, group - group // 2)]

    @pl.when(gy < ngy - 1)
    def _():
        pltpu.make_async_copy(near, near, face_recv.at[1]).wait()

    @pl.when(gy > 0)
    def _():
        pltpu.make_async_copy(far, far, face_recv.at[2]).wait()

    for x in range(cx):
        for h in range(halves):
            own = lines[x, h, pl.ds(cy - 1 if x < middle else 0, width, stride=cy), :]
            at = (x // yo) * halves + h
            fill(lefts.at[0 if x < middle else 1], (x % yo) * width, at, own)
    cut = (group // 2) * halves
    for c in range(group):
        for h in range(halves):
            at = c * halves + h
            fill(lefts.at[1 if at < cut else 0], 0, at, face_y[c, h])
    pairs[gx, gy, 1] = packed(-block_sum(couple(0, cut), width))
    pairs[gx, gy, 2] = packed(-block_sum(couple(cut, group * halves), width))

    @pl.when(gx > 0)
    def _():
        over_x(gx).wait_send()

    @pl.when(gy > 0)
    def _():
        pltpu.make_async_copy(near, near, face_send.at[1]).wait()

    @pl.when(gy < ngy - 1)
    def _():
        pltpu.make_async_copy(far, far, face_send.at[2]).wait()

    def to_y(peer):
        piece = pairs.at[gx, gy]
        return pltpu.make_async_remote_copy(
            src_ref=piece, dst_ref=piece, send_sem=pair_sem.at[0], recv_sem=pair_sem.at[1],
            device_id=(gx, peer), device_id_type=MESH,
        )

    def to_x(peer):
        piece = pairs.at[gx]
        return pltpu.make_async_remote_copy(
            src_ref=piece, dst_ref=piece, send_sem=pair_sem.at[2], recv_sem=pair_sem.at[3],
            device_id=(peer, gy), device_id_type=MESH,
        )

    def to_all(d):
        piece = diag.at[me]
        return pltpu.make_async_remote_copy(
            src_ref=piece, dst_ref=piece, send_sem=diag_sem.at[0], recv_sem=diag_sem.at[1],
            device_id=other(d), device_id_type=MESH,
        )

    def await_bytes(ref, sem):
        pltpu.make_async_copy(ref, ref, sem).wait()

    row_rest, grid_rest = pairs.at[0, pl.ds(0, ngy - 1)], pairs.at[pl.ds(0, ngx - 1)]
    for d in range(1, ngy):
        to_y(lax.rem(gy + d, ngy)).start()

    result = first

    def applied(x, slot, t):
        here, above = line_of(result, x, t), line_of(result, x, t, 1)
        up = line_of(result, x + 1, t)
        edge = jnp.where(upper_lane, 0.0, forward(here))
        beside = here[1:] + [edge]
        return [
            centre[slot, j, t * ROWS:(t + 1) * ROWS, :] * here[j] - (beside[j] + above[j] + up[j])
            for j in range(yi)
        ]

    def block(x, slot):
        for i in range(2):
            wide = expanded(3.0 + 0.5 * react[x + i])
            for j in range(yi):
                centre[slot + i, j] = wide[:, j * LANES:(j + 1) * LANES]
        for n in range(ztiles // 2):
            for i in range(2):
                two = [applied(x + i, slot + i, t) for t in (2 * n, 2 * n + 1)]
                for j in range(yi):
                    at = j * cz + n * 2 * ROWS
                    both = jnp.concatenate([two[0][j], two[1][j]], axis=0)
                    for part, value in enumerate(split(both)):
                        rights[slot + i, part, at:at + 2 * ROWS] = value
            i, (j, h) = n // len(squares), squares[n % len(squares)]
            part = result[x + i, j, ROWS + h * LANES:ROWS + (h + 1) * LANES, :].T
            lines[x + i, h, pl.ds(j, LANES, stride=yi), :] = part
            for half, value in enumerate(split(part)):
                lefts[slot + i, j * halves + h, half * LANES:(half + 1) * LANES] = value

    def multiply(slot, fresh=None):
        for i in range(2):
            total = gram[...] + jnp.dot(
                joined(lefts.at[slot + i]), joined(rights.at[slot + i]), preferred_element_type=F32
            )
            gram[...] = total if fresh is None else jnp.where(fresh, 0.0, total)

    steps = cx // 4

    @pl.loop(0, steps)
    def _(n):
        @pl.when(n == steps // 2)
        def _():
            await_bytes(row_rest, pair_sem.at[1])
            for d in range(1, ngx):
                to_x(lax.rem(gx + d, ngx)).start()

        multiply(2, n == 0)
        block(4 * n, 0)
        multiply(0)
        block(4 * n + 2, 2)

    multiply(2)

    half = strided_sum(gram[...])
    diag[me] = packed(half + half.T)

    @pl.loop(1, count)
    def _(d):
        to_all(d).start()

    await_bytes(row_rest, pair_sem.at[0])
    await_bytes(grid_rest, pair_sem.at[3])
    await_bytes(grid_rest, pair_sem.at[2])
    pairs_out[...] = pairs[...]
    all_rest = diag.at[pl.ds(0, count - 1)]
    await_bytes(all_rest, diag_sem.at[1])
    await_bytes(all_rest, diag_sem.at[0])
    diag_out[...] = diag[...]


def main(basis, reaction):
    ngx, ngy = lax.axis_size("gx"), lax.axis_size("gy")
    width, cx, cy, cz = basis.shape
    yo = LANES // width
    yi = cy // yo
    hbm = pl.BlockSpec(memory_space=pltpu.HBM)
    vmem = pl.BlockSpec(memory_space=pltpu.VMEM)
    field = [pltpu.VMEM((cx + i, yi, cz + 2 * ROWS, LANES), F32) for i in (1, 0)]
    tile = (width * width // LANES, LANES)
    return pl.pallas_call(
        functools.partial(main_kernel, ngx, ngy),
        in_specs=[hbm, hbm],
        out_specs=[vmem, vmem, vmem],
        out_shape=[
            jax.ShapeDtypeStruct((cx, cz // LANES, width, cy, LANES), F32),
            jax.ShapeDtypeStruct((ngx, ngy, 3) + tile, F32),
            jax.ShapeDtypeStruct((ngx * ngy,) + tile, F32),
        ],
        scratch_shapes=[
            pltpu.VMEM((cx, cy, cz), F32),
            pltpu.VMEM((3 * cy, yi * LANES), BF16),
            pltpu.VMEM((cx, yi, cz, LANES), F32),
            pltpu.VMEM((4, yi, cz, LANES), F32),
            *field,
            pltpu.VMEM((4, yi * cz // LANES, 2 * LANES, LANES), BF16),
            pltpu.VMEM((4, 2, yi * cz, LANES), BF16),
            pltpu.VMEM((2 * LANES, 2 * LANES), F32),
            pltpu.VMEM((LANES, LANES), F32),
            pltpu.VMEM((cz // LANES, width, cy, LANES), F32),
            pltpu.VMEM((cx // yo, cz // LANES, LANES, LANES), F32),
            pltpu.VMEM((ngx, ngy, 3) + tile, F32),
            pltpu.VMEM((ngx * ngy,) + tile, F32),
            pltpu.SemaphoreType.DMA((cx,)),
            pltpu.SemaphoreType.DMA,
            pltpu.SemaphoreType.DMA((3,)),
            pltpu.SemaphoreType.DMA((3,)),
            pltpu.SemaphoreType.DMA((4,)),
            pltpu.SemaphoreType.DMA((2,)),
        ],
        compiler_params=pltpu.CompilerParams(
            collective_id=0, has_side_effects=True, vmem_limit_bytes=40 * 2**20
        ),
        cost_estimate=pl.CostEstimate(
            flops=60 * basis.size, bytes_accessed=8 * basis.size, transcendentals=0
        ),
    )(basis, reaction)


def write_kernel(nat, pairs, diag, extended, coarse, blocks, out_sem, coarse_sem):
    width, cx, cy, cz = extended.shape
    ngx, ngy = pairs.shape[:2]

    @pl.loop(0, cx)
    def _(x):
        for h in range(cz // LANES):
            pltpu.make_async_copy(
                nat.at[x, h], extended.at[:, x, :, h * LANES:(h + 1) * LANES], out_sem
            ).start()

    nothing = jnp.zeros((width, width), F32)

    @pl.loop(0, ngx)
    def _(row):
        for col in range(ngy):
            s = row * ngy + col
            below = jnp.maximum(row - 1, 0)
            blocks[s, 0] = unpacked(diag[s], width)
            lower = unpacked(pairs[below, col, 0], width).T
            blocks[s, 1] = jnp.where(row > 0, lower, 0.0)
            blocks[s, 2] = jnp.where(row < ngx - 1, unpacked(pairs[row, col, 0], width), 0.0)
            blocks[s, 3] = nothing
            if col > 0:
                blocks[s, 3] = unpacked(pairs[row, col - 1, 1] + pairs[row, col, 2], width).T
            blocks[s, 4] = nothing
            if col < ngy - 1:
                blocks[s, 4] = unpacked(pairs[row, col, 1] + pairs[row, col + 1, 2], width)

    copy = pltpu.make_async_copy(blocks, coarse, coarse_sem)
    copy.start()
    pltpu.make_async_copy(nat, nat, out_sem).wait()
    copy.wait()


def write(nat, pairs, diag, shape):
    width = shape[0]
    vmem = pl.BlockSpec(memory_space=pltpu.VMEM)
    hbm = pl.BlockSpec(memory_space=pltpu.HBM)
    coarse = (diag.shape[0], 5, width, width)
    return pl.pallas_call(
        write_kernel,
        in_specs=[vmem, vmem, vmem],
        out_specs=[hbm, hbm],
        out_shape=[jax.ShapeDtypeStruct(shape, F32), jax.ShapeDtypeStruct(coarse, F32)],
        scratch_shapes=[
            pltpu.VMEM(coarse, F32),
            pltpu.SemaphoreType.DMA,
            pltpu.SemaphoreType.DMA,
        ],
        compiler_params=pltpu.CompilerParams(vmem_limit_bytes=16 * 2**20),
    )(nat, pairs, diag)


def on_device(basis, reaction):
    return write(*main(basis, reaction), basis.shape)


def solution(mesh):
    placed = (P(None, "gx", "gy", None), P("gx", "gy", None))
    return jax.shard_map(
        on_device,
        mesh=mesh,
        in_specs=placed,
        out_specs=(P(None, "gx", "gy", None), P()),
        check_vma=False,
    )
```

```python
import functools

import jax
import jax.numpy as jnp
from jax import lax
from jax.experimental import pallas as pl
from jax.experimental.pallas import tpu as pltpu
from jax.sharding import PartitionSpec as P

SWEEPS = 4
OMEGA = 0.8
ROWS = 8
LANES = 128
MESH = pl.DeviceIdType.MESH
F32 = jnp.float32
BF16 = jnp.bfloat16


def split(value):
    high = value.astype(BF16)
    low = (value - high.astype(F32)).astype(BF16)
    return high, low


def thirds(value):
    first = value.astype(BF16)
    rest = value - first.astype(F32)
    second = rest.astype(BF16)
    third = (rest - second.astype(F32)).astype(BF16)
    return jnp.concatenate([first, second, third], axis=0)


def combined(wide):
    half = wide.shape[0] // 2
    return wide[:half, :half] + wide[:half, half:] + wide[half:, :half]


def block_sum(wide, width):
    full = combined(wide)
    total = full[:width, :width]
    for i in range(width, full.shape[0], width):
        total = total + full[i:i + width, i:i + width]
    return total


def packed(block):
    rows = block.shape[0] * block.shape[1] // LANES
    return jnp.concatenate(
        [block[i:i + rows] for i in range(0, block.shape[0], rows)], axis=1
    )


def unpacked(tile, width):
    return jnp.concatenate(
        [tile[:, i:i + width] for i in range(0, LANES, width)], axis=0
    )


def main_kernel(
    ngx, ngy, basis, reaction, nat, pairs_out, diag_out,
    react, spread, weight, centre, first, second, lefts, rights,
    gram, square, face_x, face_y, pairs, diag,
    in_sem, react_sem, face_send, face_recv, pair_sem, diag_sem,
):
    width, cx, cy, cz = basis.shape
    yo = LANES // width
    yi = cy // yo
    group = cx // yo
    halves = cz // LANES
    ztiles = cz // ROWS
    gx, gy = lax.axis_index("gx"), lax.axis_index("gy")

    lines = nat.reshape(cx, halves, width * cy, LANES)
    count = ngx * ngy
    me = gx * ngy + gy

    columns = [lax.rem(gx + d, ngx) for d in range(1, ngx)] + [gx]
    planes = [lax.rem(gy + d, ngy) for d in range(1, ngy)] + [gy]
    others = [(column, plane) for column in columns for plane in planes][:-1]

    load = pltpu.make_async_copy(reaction, react, react_sem)
    load.start()

    @pl.loop(0, cx)
    def _(x):
        for h in range(halves):
            pltpu.make_async_copy(
                basis.at[:, x, :, h * LANES:(h + 1) * LANES], nat.at[x, h], in_sem.at[x]
            ).start()

    barrier = pltpu.get_barrier_semaphore()
    for peer in others:
        pl.semaphore_signal(barrier, inc=1, device_id=peer, device_id_type=MESH)

    def over_x(peer):
        return pltpu.make_async_remote_copy(
            src_ref=nat.at[0], dst_ref=face_x, send_sem=face_send.at[0], recv_sem=face_recv.at[0],
            device_id=(peer, gy), device_id_type=MESH,
        )

    def over_y(x, upper, peer):
        return pltpu.make_async_remote_copy(
            src_ref=nat.at[x, :, :, cy - 1 if upper else 0, :],
            dst_ref=face_y.at[x // yo, :, pl.ds(lax.rem(x, yo) * width, width), :],
            send_sem=face_send.at[1 + upper], recv_sem=face_recv.at[1 + upper],
            device_id=(gx, peer), device_id_type=MESH,
        )

    middle = (group // 2) * yo

    rows = lax.broadcasted_iota(jnp.int32, (cy, yi * LANES), 0)
    cols = lax.broadcasted_iota(jnp.int32, (cy, yi * LANES), 1)
    chosen = rows == lax.rem(cols, yo) * yi + cols // LANES
    pick = jnp.where(chosen, 1.0, 0.0).astype(BF16)
    spread[...] = jnp.concatenate([pick, pick, pick], axis=0)

    def expanded(values):
        return lax.dot_general(
            thirds(values), spread[...], (((0,), (0,)), ((), ())), preferred_element_type=F32
        )

    line = lax.broadcasted_iota(jnp.int32, (cy, cz), 0)
    face_row = (line == 0) | (line == cy - 1)
    blank = jnp.zeros((ROWS, LANES), F32)
    def weigh(x):
        wide = expanded(jnp.where(face_row, 0.0, OMEGA / (6.0 + react[x])))
        for j in range(yi):
            weight[x, j] = wide[:, j * LANES:(j + 1) * LANES]

    @pl.loop(0, ztiles + 2)
    def _(t):
        for j in range(yi):
            first[cx, j, pl.ds(t * ROWS, ROWS), :] = blank

    @pl.loop(0, cx)
    def _(x):
        for j in range(yi):
            for buffer in (first, second):
                buffer[x, j, 0:ROWS, :] = blank
                buffer[x, j, cz + ROWS:cz + 2 * ROWS, :] = blank

    gram[...] = jnp.zeros_like(gram)

    lane = lax.broadcasted_iota(jnp.int32, (ROWS, LANES), 1)
    keep = [jnp.full((ROWS, LANES), 1.0 - OMEGA, F32) for _ in range(yi)]
    upper_lane = lax.rem(lane, yo) == yo - 1
    keep[0] = jnp.where(lax.rem(lane, yo) == 0, 1.0, keep[0])
    keep[yi - 1] = jnp.where(upper_lane, 1.0, keep[yi - 1])

    def land(x):
        pltpu.make_async_copy(nat.at[x], nat.at[x], in_sem.at[x]).wait()

    def take_in(x, j, h):
        part = lines[x, h, pl.ds(j, LANES, stride=yi), :]
        first[x, j, ROWS + h * LANES:ROWS + (h + 1) * LANES, :] = part.T

    squares = [(j, h) for j in range(yi) for h in range(halves)]

    def line_of(ref, x, t, shift=0):
        return [ref[x, j, pl.ds(ROWS + t * ROWS + shift, ROWS), :] for j in range(yi)]

    def forward(values):
        return pltpu.roll(values[0], LANES - 1, 1)

    def backward(values):
        return pltpu.roll(values[yi - 1], 1, 1)

    def diagonals(here, up):
        inner = [here[j] + up[j + 1] for j in range(yi - 1)]
        return [backward(here) + up[0]] + inner + [here[yi - 1] + forward(up)]

    def finish(source, target, x, t, here, total):
        below, above = line_of(source, x, t, -1), line_of(source, x, t, 1)
        for j in range(yi):
            around = total[j] + (below[j] + above[j])
            target[x, j, pl.ds(ROWS + t * ROWS, ROWS), :] = (
                keep[j] * here[j] + weight[x, j, pl.ds(t * ROWS, ROWS), :] * around
            )

    def sweep_pair(source, target, x, t):
        field = [line_of(source, x + i, t) for i in range(4)]
        for i in range(1, 3):
            down, here, up = field[i - 1:i + 2]
            near = [backward(here)] + here + [forward(here)]
            total = [(down[j] + up[j]) + (near[j] + near[j + 2]) for j in range(yi)]
            finish(source, target, x + i, t, here, total)

    def sweep(source, target):
        @pl.loop(0, ztiles, unroll=2)
        def _(t):
            here = line_of(source, 1, t)
            old = diagonals(line_of(source, 0, t), here)
            for x in range(1, cx - 1):
                up = line_of(source, x + 1, t)
                new = diagonals(here, up)
                total = [old[j + 1] + new[j] for j in range(yi)]
                finish(source, target, x, t, here, total)
                old, here = new, up

    for x in range(4):
        land(x)
        for at in squares:
            take_in(x, *at)

    load.wait()
    for x in (1, 2):
        weigh(x)
    each = ztiles // (2 * len(squares))

    @pl.loop(0, cx - 4, step=2)
    def _(x):
        land(x + 4)
        land(x + 5)
        weigh(x + 3)
        weigh(x + 4)
        for i in range(2):
            for n, at in enumerate(squares):
                take_in(x + 4 + i, *at)
                for m in range(each):
                    sweep_pair(first, second, x, (i * len(squares) + n) * each + m)

    pl.semaphore_wait(barrier, count - 1)

    @pl.when(gx > 0)
    def _():
        over_x(gx - 1).start()

    @pl.when(gy > 0)
    def _():
        @pl.loop(0, middle)
        def _(x):
            over_y(x, 0, gy - 1).start()

    @pl.when(gy < ngy - 1)
    def _():
        @pl.loop(middle, cx)
        def _(x):
            over_y(x, 1, gy + 1).start()

    for t in range(ztiles):
        sweep_pair(first, second, cx - 4, t)

    @pl.loop(0, ztiles)
    def _(t):
        for x in (0, cx - 1):
            for j, value in enumerate(line_of(first, x, t)):
                second[x, j, pl.ds(ROWS + t * ROWS, ROWS), :] = value

    sweep(second, first)
    sweep(first, second)
    sweep(second, first)

    def joined(ref, start=0, stop=None):
        stop = ref.shape[0] if stop is None else stop
        return jnp.concatenate([ref[i] for i in range(start, stop)], axis=1)

    def couple(slot, start, stop):
        return lax.dot_general(
            joined(lefts.at[slot], start, stop), joined(lefts.at[slot + 1], start, stop),
            (((1,), (1,)), ((), ())), preferred_element_type=F32,
        )

    def strided_sum(wide):
        square[...] = combined(wide)
        turned = jnp.concatenate(
            [square[pl.ds(g, width, stride=yo), :] for g in range(yo)], axis=0
        ).T
        square[...] = turned
        total = square[pl.ds(0, width, stride=yo), :][:, :width]
        for g in range(1, yo):
            total = total + square[pl.ds(g, width, stride=yo), :][:, g * width:(g + 1) * width]
        return total

    def fill(ref, row, column, value):
        size = value.shape[0]
        for half, part in enumerate(split(value)):
            ref[column, half * LANES + row:half * LANES + row + size] = part

    @pl.when(gx < ngx - 1)
    def _():
        over_x(gx).wait_recv()

    near, far = face_y.at[pl.ds(0, group // 2)], face_y.at[pl.ds(group // 2, group - group // 2)]

    @pl.when(gy < ngy - 1)
    def _():
        pltpu.make_async_copy(near, near, face_recv.at[1]).wait()

    @pl.when(gy > 0)
    def _():
        pltpu.make_async_copy(far, far, face_recv.at[2]).wait()

    for n, (j, h) in enumerate(squares):
        fill(lefts.at[0], 0, n, face_x.reshape(halves, width * cy, LANES)[h, pl.ds(j, LANES, stride=yi), :])
        fill(lefts.at[1], 0, n, lines[cx - 1, h, pl.ds(j, LANES, stride=yi), :])
    pairs[gx, gy, 0] = packed(-strided_sum(couple(0, 0, len(squares))))

    for x in range(cx):
        for h in range(halves):
            own = lines[x, h, pl.ds(cy - 1 if x < middle else 0, width, stride=cy), :]
            at = (x // yo) * halves + h
            fill(lefts.at[2 if x < middle else 3], (x % yo) * width, at, own)
    cut = (group // 2) * halves
    for c in range(group):
        for h in range(halves):
            at = c * halves + h
            fill(lefts.at[3 if at < cut else 2], 0, at, face_y[c, h])
    pairs[gx, gy, 1] = packed(-block_sum(couple(2, 0, cut), width))
    pairs[gx, gy, 2] = packed(-block_sum(couple(2, cut, group * halves), width))

    @pl.when(gx > 0)
    def _():
        over_x(gx).wait_send()

    @pl.when(gy > 0)
    def _():
        pltpu.make_async_copy(near, near, face_send.at[1]).wait()

    @pl.when(gy < ngy - 1)
    def _():
        pltpu.make_async_copy(far, far, face_send.at[2]).wait()

    def to_y(peer):
        piece = pairs.at[gx, gy]
        return pltpu.make_async_remote_copy(
            src_ref=piece, dst_ref=piece, send_sem=pair_sem.at[0], recv_sem=pair_sem.at[1],
            device_id=(gx, peer), device_id_type=MESH,
        )

    def to_x(peer):
        piece = pairs.at[gx]
        return pltpu.make_async_remote_copy(
            src_ref=piece, dst_ref=piece, send_sem=pair_sem.at[2], recv_sem=pair_sem.at[3],
            device_id=(peer, gy), device_id_type=MESH,
        )

    def to_other(peer):
        piece = diag.at[me]
        return pltpu.make_async_remote_copy(
            src_ref=piece, dst_ref=piece, send_sem=diag_sem.at[0], recv_sem=diag_sem.at[1],
            device_id=peer, device_id_type=MESH,
        )

    def await_bytes(ref, sem):
        pltpu.make_async_copy(ref, ref, sem).wait()

    row_rest, grid_rest = pairs.at[0, pl.ds(0, ngy - 1)], pairs.at[pl.ds(0, ngx - 1)]
    for plane in planes[:-1]:
        to_y(plane).start()

    result = first

    def applied(x, slot, t):
        here, above = line_of(result, x, t), line_of(result, x, t, 1)
        up = line_of(result, x + 1, t)
        edge = jnp.where(upper_lane, 0.0, forward(here))
        beside = here[1:] + [edge]
        return [
            centre[slot, j, t * ROWS:(t + 1) * ROWS, :] * here[j] - (beside[j] + above[j] + up[j])
            for j in range(yi)
        ]

    def block(x, slot):
        for i in range(2):
            wide = expanded(3.0 + 0.5 * react[x + i])
            for j in range(yi):
                centre[slot + i, j] = wide[:, j * LANES:(j + 1) * LANES]
        for n in range(ztiles // 2):
            for i in range(2):
                two = [applied(x + i, slot + i, t) for t in (2 * n, 2 * n + 1)]
                for j in range(yi):
                    at = j * cz + n * 2 * ROWS
                    both = jnp.concatenate([two[0][j], two[1][j]], axis=0)
                    for part, value in enumerate(split(both)):
                        rights[slot + i, part, at:at + 2 * ROWS] = value
            i, (j, h) = n // len(squares), squares[n % len(squares)]
            part = result[x + i, j, ROWS + h * LANES:ROWS + (h + 1) * LANES, :].T
            lines[x + i, h, pl.ds(j, LANES, stride=yi), :] = part
            for half, value in enumerate(split(part)):
                lefts[slot + i, j * halves + h, half * LANES:(half + 1) * LANES] = value

    def multiply(slot, fresh=None):
        for i in range(2):
            total = gram[...] + jnp.dot(
                joined(lefts.at[slot + i]), joined(rights.at[slot + i]), preferred_element_type=F32
            )
            gram[...] = total if fresh is None else jnp.where(fresh, 0.0, total)

    steps = cx // 4

    @pl.loop(0, steps)
    def _(n):
        @pl.when(n == steps // 2)
        def _():
            await_bytes(row_rest, pair_sem.at[1])
            for column in columns[:-1]:
                to_x(column).start()

        multiply(2, n == 0)
        block(4 * n, 0)
        multiply(0)
        block(4 * n + 2, 2)

    multiply(2)

    half = strided_sum(gram[...])
    diag[me] = packed(half + half.T)

    for peer in others:
        to_other(peer).start()

    await_bytes(row_rest, pair_sem.at[0])
    await_bytes(grid_rest, pair_sem.at[3])
    await_bytes(grid_rest, pair_sem.at[2])
    pairs_out[...] = pairs[...]
    all_rest = diag.at[pl.ds(0, count - 1)]
    await_bytes(all_rest, diag_sem.at[1])
    await_bytes(all_rest, diag_sem.at[0])
    diag_out[...] = diag[...]


def main(basis, reaction):
    ngx, ngy = lax.axis_size("gx"), lax.axis_size("gy")
    width, cx, cy, cz = basis.shape
    yo = LANES // width
    yi = cy // yo
    hbm = pl.BlockSpec(memory_space=pltpu.HBM)
    vmem = pl.BlockSpec(memory_space=pltpu.VMEM)
    field = [pltpu.VMEM((cx + i, yi, cz + 2 * ROWS, LANES), F32) for i in (1, 0)]
    tile = (width * width // LANES, LANES)
    return pl.pallas_call(
        functools.partial(main_kernel, ngx, ngy),
        in_specs=[hbm, hbm],
        out_specs=[vmem, vmem, vmem],
        out_shape=[
            jax.ShapeDtypeStruct((cx, cz // LANES, width, cy, LANES), F32),
            jax.ShapeDtypeStruct((ngx, ngy, 3) + tile, F32),
            jax.ShapeDtypeStruct((ngx * ngy,) + tile, F32),
        ],
        scratch_shapes=[
            pltpu.VMEM((cx, cy, cz), F32),
            pltpu.VMEM((3 * cy, yi * LANES), BF16),
            pltpu.VMEM((cx, yi, cz, LANES), F32),
            pltpu.VMEM((4, yi, cz, LANES), F32),
            *field,
            pltpu.VMEM((4, yi * cz // LANES, 2 * LANES, LANES), BF16),
            pltpu.VMEM((4, 2, yi * cz, LANES), BF16),
            pltpu.VMEM((2 * LANES, 2 * LANES), F32),
            pltpu.VMEM((LANES, LANES), F32),
            pltpu.VMEM((cz // LANES, width, cy, LANES), F32),
            pltpu.VMEM((cx // yo, cz // LANES, LANES, LANES), F32),
            pltpu.VMEM((ngx, ngy, 3) + tile, F32),
            pltpu.VMEM((ngx * ngy,) + tile, F32),
            pltpu.SemaphoreType.DMA((cx,)),
            pltpu.SemaphoreType.DMA,
            pltpu.SemaphoreType.DMA((3,)),
            pltpu.SemaphoreType.DMA((3,)),
            pltpu.SemaphoreType.DMA((4,)),
            pltpu.SemaphoreType.DMA((2,)),
        ],
        compiler_params=pltpu.CompilerParams(
            collective_id=0, has_side_effects=True, vmem_limit_bytes=40 * 2**20
        ),
        cost_estimate=pl.CostEstimate(
            flops=60 * basis.size, bytes_accessed=8 * basis.size, transcendentals=0
        ),
    )(basis, pltpu.with_memory_space_constraint(reaction, pltpu.HBM))


def write_kernel(nat, pairs, diag, extended, coarse, blocks, out_sem, coarse_sem):
    width, cx, cy, cz = extended.shape
    ngx, ngy = pairs.shape[:2]

    @pl.loop(0, cx)
    def _(x):
        for h in range(cz // LANES):
            pltpu.make_async_copy(
                nat.at[x, h], extended.at[:, x, :, h * LANES:(h + 1) * LANES], out_sem
            ).start()

    nothing = jnp.zeros((width, width), F32)

    @pl.loop(0, ngx)
    def _(row):
        for col in range(ngy):
            s = row * ngy + col
            below = jnp.maximum(row - 1, 0)
            blocks[s, 0] = unpacked(diag[s], width)
            lower = unpacked(pairs[below, col, 0], width).T
            blocks[s, 1] = jnp.where(row > 0, lower, 0.0)
            blocks[s, 2] = jnp.where(row < ngx - 1, unpacked(pairs[row, col, 0], width), 0.0)
            blocks[s, 3] = nothing
            if col > 0:
                blocks[s, 3] = unpacked(pairs[row, col - 1, 1] + pairs[row, col, 2], width).T
            blocks[s, 4] = nothing
            if col < ngy - 1:
                blocks[s, 4] = unpacked(pairs[row, col, 1] + pairs[row, col + 1, 2], width)

    copy = pltpu.make_async_copy(blocks, coarse, coarse_sem)
    copy.start()
    pltpu.make_async_copy(nat, nat, out_sem).wait()
    copy.wait()


def write(nat, pairs, diag, shape):
    width = shape[0]
    vmem = pl.BlockSpec(memory_space=pltpu.VMEM)
    hbm = pl.BlockSpec(memory_space=pltpu.HBM)
    coarse = (diag.shape[0], 5, width, width)
    return pl.pallas_call(
        write_kernel,
        in_specs=[vmem, vmem, vmem],
        out_specs=[hbm, hbm],
        out_shape=[jax.ShapeDtypeStruct(shape, F32), jax.ShapeDtypeStruct(coarse, F32)],
        scratch_shapes=[
            pltpu.VMEM(coarse, F32),
            pltpu.SemaphoreType.DMA,
            pltpu.SemaphoreType.DMA,
        ],
        compiler_params=pltpu.CompilerParams(vmem_limit_bytes=16 * 2**20),
    )(nat, pairs, diag)


def on_device(basis, reaction):
    return write(*main(basis, reaction), basis.shape)


def solution(mesh):
    placed = (P(None, "gx", "gy", None), P("gx", "gy", None))
    return jax.shard_map(
        on_device,
        mesh=mesh,
        in_specs=placed,
        out_specs=(P(None, "gx", "gy", None), P()),
        check_vma=False,
    )
```
